32 devices in a mesh: dp: 2 (over x), tp: 4 (over z), sp: 4 (over y, core).
Axes of the slice: x: 2, y: 2, z: 4, core: 2. Of those that a mesh axis runs over, the one named last changes fastest.
Arguments:
- step_emb: bfloat16 [4, 4, 768], P(None, 'dp'), parts along dimension 1
- v_cache: bfloat16 [2, 4, 16384, 768], P(None, 'dp', 'sp', 'tp'), parts along dimension 1
- z_cache: bfloat16 [2, 4, 16384, 768], P(None, 'dp', 'sp', 'tp'), parts along dimension 1
- short_state: bfloat16 [2, 4, 2, 3, 768], P(None, 'dp', None, None, 'tp'), parts along dimension 1
- w_in: bfloat16 [2, 768, 3, 768], P(None, None, None, 'tp')
- b_in: float32 [2, 3, 768], P(None, None, 'tp')
- short_taps: float32 [2, 3, 3, 768], P(None, None, None, 'tp')
- long_filt: float32 [2, 2, 16384, 768], P(None, None, None, 'tp')
- skip_gain: float32 [2, 2, 768], P(None, None, 'tp')
- w_out: bfloat16 [2, 768, 768], P(None, 'tp')
- b_out: float32 [2, 768], replicated
- w_up: bfloat16 [2, 768, 3072], P(None, None, 'tp')
- w_down: bfloat16 [2, 3072, 768], P(None, 'tp')
Outputs:
- output 1: float32 [4, 4, 768], P(None, 'dp'), parts along dimension 1
- output 2: bfloat16 [2, 4, 16384, 768], P(None, 'dp', 'sp', 'tp'), parts along dimension 1
- output 3: bfloat16 [2, 4, 16384, 768], P(None, 'dp', 'sp', 'tp'), parts along dimension 1
- output 4: bfloat16 [2, 4, 2, 3, 768], P(None, 'dp', None, None, 'tp'), parts along dimension 1
There are 2 independent parts. The reference program is written for one: setup_inputs(seed, part) draws one part's arguments, and reference() takes and returns one part's arrays. A program takes and returns all parts, laid end to end along the dimension named above; an argument that names none is the same for every part.
All inputs are finite; a program needn't handle non-finite values.
Results may differ from the reference program's by a relative error of at most 0.010954.
Values sent between devices are 32-bit elements.
A program may use at most 1 GiB of HBM per device.

```python
import jax
import jax.numpy as jnp
from jax import lax

MODEL_DIM = 768
MLP_DIM = 3072
NUM_SEQ = 2
CACHE_LEN = 16384
NUM_STEPS = 4
NUM_LAYERS = 2
START_POS = CACHE_LEN * 3 // 4


def setup_inputs(seed: int = 0, part: int = 0) -> dict:
    root_key = jax.random.key(seed)
    part_root, shared_root = jax.random.split(root_key)
    part_keys = jax.random.split(jax.random.fold_in(part_root, part), 4)
    shared_keys = jax.random.split(shared_root, 9)
    filled_mask = (jnp.arange(CACHE_LEN) < START_POS)[None, None, :, None]
    lag_pos = jnp.arange(CACHE_LEN).astype(jnp.float32)
    decay_rows = jnp.exp(-0.5 * lag_pos / CACHE_LEN)[:, None]
    cache_shape = (NUM_LAYERS, NUM_SEQ, CACHE_LEN, MODEL_DIM)
    step_emb = jax.random.normal(part_keys[0], (NUM_STEPS, NUM_SEQ, MODEL_DIM), jnp.float32)
    v_cache = jax.random.normal(part_keys[1], cache_shape, jnp.float32) * filled_mask
    z_cache = jax.random.normal(part_keys[2], cache_shape, jnp.float32) * filled_mask
    short_state = jax.random.normal(part_keys[3], (NUM_LAYERS, NUM_SEQ, 2, 3, MODEL_DIM), jnp.float32)
    w_in = jax.random.normal(shared_keys[0], (NUM_LAYERS, MODEL_DIM, 3, MODEL_DIM), jnp.float32) * MODEL_DIM ** -0.5
    b_in = 0.5 * jax.random.normal(shared_keys[1], (NUM_LAYERS, 3, MODEL_DIM), jnp.float32)
    short_taps = 0.6 * jax.random.normal(shared_keys[2], (NUM_LAYERS, 3, 3, MODEL_DIM), jnp.float32)
    long_filt = jax.random.normal(shared_keys[3], (NUM_LAYERS, 2, CACHE_LEN, MODEL_DIM), jnp.float32) * decay_rows * (1.4 * CACHE_LEN ** -0.5)
    skip_gain = 0.6 * jax.random.normal(shared_keys[4], (NUM_LAYERS, 2, MODEL_DIM), jnp.float32)
    w_out = jax.random.normal(shared_keys[5], (NUM_LAYERS, MODEL_DIM, MODEL_DIM), jnp.float32) * MODEL_DIM ** -0.5
    b_out = 0.5 * jax.random.normal(shared_keys[6], (NUM_LAYERS, MODEL_DIM), jnp.float32)
    w_up = jax.random.normal(shared_keys[7], (NUM_LAYERS, MODEL_DIM, MLP_DIM), jnp.float32) * MODEL_DIM ** -0.5
    w_down = jax.random.normal(shared_keys[8], (NUM_LAYERS, MLP_DIM, MODEL_DIM), jnp.float32) * (1.5 * MLP_DIM ** -0.5)
    return {
        "step_emb": step_emb.astype(jnp.bfloat16),
        "v_cache": v_cache.astype(jnp.bfloat16),
        "z_cache": z_cache.astype(jnp.bfloat16),
        "short_state": short_state.astype(jnp.bfloat16),
        "w_in": w_in.astype(jnp.bfloat16),
        "b_in": b_in,
        "short_taps": short_taps,
        "long_filt": long_filt,
        "skip_gain": skip_gain,
        "w_out": w_out.astype(jnp.bfloat16),
        "b_out": b_out,
        "w_up": w_up.astype(jnp.bfloat16),
        "w_down": w_down.astype(jnp.bfloat16),
    }


def layer_norm(rows_in):
    mean_val = jnp.mean(rows_in, axis=-1, keepdims=True)
    centered = rows_in - mean_val
    var_val = jnp.mean(centered * centered, axis=-1, keepdims=True)
    return centered * lax.rsqrt(var_val + 1e-5)


def long_conv(cache_rows, filt_rows, pos_now):
    lag_pos = pos_now - jnp.arange(CACHE_LEN)
    taps_now = jnp.take(filt_rows, jnp.maximum(lag_pos, 0), axis=0)
    taps_now = jnp.where((lag_pos >= 0)[:, None], taps_now, 0.0)
    return jnp.sum(cache_rows.astype(jnp.float32) * taps_now[None], axis=1)


def reference(step_emb, v_cache, z_cache, short_state, w_in, b_in, short_taps, long_filt, skip_gain, w_out, b_out, w_up, w_down):
    def one_step(carry, step_in):
        v_list, z_list, state_list = carry
        emb_row, step_idx = step_in
        pos_now = START_POS + step_idx
        hidden = emb_row.astype(jnp.float32)
        new_v = []
        new_z = []
        new_state = []
        for layer_idx in range(NUM_LAYERS):
            normed = layer_norm(hidden).astype(jnp.bfloat16)
            w_flat = w_in[layer_idx].reshape(MODEL_DIM, 3 * MODEL_DIM)
            proj_row = jnp.dot(normed, w_flat, preferred_element_type=jnp.float32).reshape(-1, 3, MODEL_DIM)
            proj_row = (proj_row + b_in[layer_idx]).astype(jnp.bfloat16)
            prev_state = state_list[layer_idx]
            tap_rows = short_taps[layer_idx]
            mixed_rows = (tap_rows[0] * proj_row.astype(jnp.float32)
                          + tap_rows[1] * prev_state[:, 1].astype(jnp.float32)
                          + tap_rows[2] * prev_state[:, 0].astype(jnp.float32))
            new_state.append(jnp.stack([prev_state[:, 1], proj_row], axis=1))
            value_row = mixed_rows[:, 2].astype(jnp.bfloat16)
            v_layer = lax.dynamic_update_slice(v_list[layer_idx], value_row[:, None, :], (0, pos_now, 0))
            long_one = long_conv(v_layer, long_filt[layer_idx, 0], pos_now) + skip_gain[layer_idx, 0] * value_row.astype(jnp.float32)
            z_row = (mixed_rows[:, 0] * long_one).astype(jnp.bfloat16)
            z_layer = lax.dynamic_update_slice(z_list[layer_idx], z_row[:, None, :], (0, pos_now, 0))
            long_two = long_conv(z_layer, long_filt[layer_idx, 1], pos_now) + skip_gain[layer_idx, 1] * z_row.astype(jnp.float32)
            y_row = (mixed_rows[:, 1] * long_two).astype(jnp.bfloat16)
            hidden = hidden + jnp.dot(y_row, w_out[layer_idx], preferred_element_type=jnp.float32) + b_out[layer_idx]
            inner_act = jax.nn.gelu(jnp.dot(layer_norm(hidden).astype(jnp.bfloat16), w_up[layer_idx], preferred_element_type=jnp.float32)).astype(jnp.bfloat16)
            hidden = hidden + jnp.dot(inner_act, w_down[layer_idx], preferred_element_type=jnp.float32)
            new_v.append(v_layer)
            new_z.append(z_layer)
        return (tuple(new_v), tuple(new_z), tuple(new_state)), hidden

    init_carry = (
        tuple(v_cache[layer_idx] for layer_idx in range(NUM_LAYERS)),
        tuple(z_cache[layer_idx] for layer_idx in range(NUM_LAYERS)),
        tuple(short_state[layer_idx] for layer_idx in range(NUM_LAYERS)),
    )
    final_carry, hiddens = lax.scan(one_step, init_carry, (step_emb, jnp.arange(NUM_STEPS)))
    v_out, z_out, state_out = final_carry
    return (hiddens, jnp.stack(v_out), jnp.stack(z_out), jnp.stack(state_out))
```

```python
import jax
import jax.numpy as jnp
from jax import lax
from jax.sharding import PartitionSpec as P

NUM_STEPS = 4
NUM_LAYERS = 2


def layer_norm(rows_in):
    mean_val = jnp.mean(rows_in, axis=-1, keepdims=True)
    centered = rows_in - mean_val
    var_val = jnp.mean(centered * centered, axis=-1, keepdims=True)
    return centered * lax.rsqrt(var_val + 1e-5)


def solution(mesh):
    sp_size = mesh.shape["sp"]

    def device_fn(step_emb, v_cache, z_cache, short_state, w_in, b_in, short_taps, long_filt, skip_gain, w_out, b_out, w_up, w_down):
        shard_len = v_cache.shape[2]
        cache_len = shard_len * sp_size
        start_pos = cache_len * 3 // 4
        sp_idx = lax.axis_index("sp")
        first = jnp.maximum(start_pos - shard_len * (sp_idx + 1), 0)
        window = lax.dynamic_slice_in_dim(long_filt, first, shard_len + 128, axis=2)
        rev = window[:, :, ::-1]
        live = (sp_idx * shard_len < start_pos)
        hist_v = []
        hist_z = []
        for j in range(NUM_STEPS):
            begin = 127 - j
            taps = rev[:, :, begin:begin + shard_len]
            hist_v.append(jnp.sum(v_cache * taps[:, 0][:, None], axis=2))
            hist_z.append(jnp.sum(z_cache * taps[:, 1][:, None], axis=2))
        hist = jnp.stack([jnp.stack(hist_v), jnp.stack(hist_z)])
        hist = lax.psum(jnp.where(live, hist, 0.0), "sp")
        hidden = step_emb.astype(jnp.float32)
        new_v = []
        new_z = []
        states = []
        for layer in range(NUM_LAYERS):
            normed = layer_norm(hidden).astype(jnp.bfloat16)
            proj = jnp.einsum("tbd,dgc->tbgc", normed, w_in[layer], preferred_element_type=jnp.float32)
            proj = (proj + b_in[layer]).astype(jnp.bfloat16)
            seq = jnp.concatenate([short_state[layer, :, 0][None], short_state[layer, :, 1][None], proj], axis=0)
            taps = short_taps[layer]
            seqf = seq.astype(jnp.float32)
            mixed = taps[0] * seqf[2:] + taps[1] * seqf[1:-1] + taps[2] * seqf[:-2]
            states.append(jnp.stack([seq[-2], seq[-1]], axis=1))
            value = mixed[:, :, 2].astype(jnp.bfloat16)

            def conv_rows(base, rows_of, which):
                outs = []
                for j in range(NUM_STEPS):
                    total = base[j]
                    for i in range(j + 1):
                        total = total + long_filt[layer, which, j - i] * rows_of[i].astype(jnp.float32)
                    outs.append(total + skip_gain[layer, which] * rows_of[j].astype(jnp.float32))
                return jnp.stack(outs)

            long_one = conv_rows(hist[0, :, layer], value, 0)
            z_rows = (mixed[:, :, 0] * long_one).astype(jnp.bfloat16)
            long_two = conv_rows(hist[1, :, layer], z_rows, 1)
            y_rows = (mixed[:, :, 1] * long_two).astype(jnp.bfloat16)
            mix_out = lax.psum(jnp.einsum("tbc,cd->tbd", y_rows, w_out[layer], preferred_element_type=jnp.float32), "tp")
            hidden = hidden + mix_out + b_out[layer]
            inner = jax.nn.gelu(jnp.einsum("tbd,df->tbf", layer_norm(hidden).astype(jnp.bfloat16), w_up[layer], preferred_element_type=jnp.float32)).astype(jnp.bfloat16)
            hidden = hidden + lax.psum(jnp.einsum("tbf,fd->tbd", inner, w_down[layer], preferred_element_type=jnp.float32), "tp")
            new_v.append(jnp.swapaxes(value, 0, 1))
            new_z.append(jnp.swapaxes(z_rows, 0, 1))

        is_owner = sp_idx == start_pos // shard_len
        at = start_pos % shard_len

        def put(cache, rows):
            old = cache[:, :, at:at + NUM_STEPS]
            return cache.at[:, :, at:at + NUM_STEPS].set(jnp.where(is_owner, jnp.stack(rows), old))

        return (hidden, put(v_cache, new_v), put(z_cache, new_z), jnp.stack(states))

    specs_in = (
        P(None, "dp", None),
        P(None, "dp", "sp", "tp"),
        P(None, "dp", "sp", "tp"),
        P(None, "dp", None, None, "tp"),
        P(None, None, None, "tp"),
        P(None, None, "tp"),
        P(None, None, None, "tp"),
        P(None, None, None, "tp"),
        P(None, None, "tp"),
        P(None, "tp", None),
        P(None, None),
        P(None, None, "tp"),
        P(None, "tp", None),
    )
    specs_out = (
        P(None, "dp", None),
        P(None, "dp", "sp", "tp"),
        P(None, "dp", "sp", "tp"),
        P(None, "dp", None, None, "tp"),
    )
    return jax.shard_map(device_fn, mesh=mesh, in_specs=specs_in, out_specs=specs_out, check_vma=False)
```

```python
import functools

import jax
import jax.numpy as jnp
from jax import lax
from jax.experimental import pallas as pl
from jax.experimental.pallas import tpu as pltpu
from jax.sharding import PartitionSpec as P

STEPS = 4
LAYERS = 2
SEQ = 2
ROWS = STEPS * SEQ
LANES = 128
CHUNKS = 4
MESH = pl.DeviceIdType.MESH


def layer_norm(rows_in):
    mean_val = jnp.mean(rows_in, axis=-1, keepdims=True)
    centered = rows_in - mean_val
    var_val = jnp.mean(centered * centered, axis=-1, keepdims=True)
    return centered * lax.rsqrt(var_val + 1e-5)


def kernel(e_hbm, v_hbm, z_hbm, st_hbm, win_hbm, bin_hbm, tap_hbm, h_hbm, skip_hbm, wout_hbm, bout_hbm, wup_hbm, wdown_hbm,
           hid_out, v_ref, z_ref, st_out,
           e_ref, st_ref, win, bin_ref, tap_ref, h_ref, lag_ref, skip_ref, wout, bout_ref, wup, wdown,
           acc, st8, newrow, hx, ar,
           small_sem, chunk_sem, w_sem, hsend, hrecv, asend, arecv, hid_sem):
    tp = lax.axis_index("tp")
    sp = lax.axis_index("sp")
    chan, shard_len = v_hbm.shape[2], v_hbm.shape[3]
    tiles = shard_len // LANES
    rows_per = chan // CHUNKS
    peers = [({"tp": lax.rem(tp + d, 4)}) for d in (1, 2, 3)]
    sp_peers = [({"sp": lax.rem(sp + d, 4)}) for d in (1, 2, 3)]

    barrier = pltpu.get_barrier_semaphore()
    for peer in peers + sp_peers:
        pl.semaphore_signal(barrier, inc=1, device_id=peer, device_id_type=MESH)

    smalls = [pltpu.make_async_copy(src, dst, small_sem.at[n]) for n, (src, dst) in enumerate((
        (e_hbm, e_ref), (st_hbm, st_ref), (bin_hbm, bin_ref), (tap_hbm, tap_ref), (skip_hbm, skip_ref), (bout_hbm, bout_ref),
        (h_hbm.at[:, :, :, pl.ds(0, LANES)], lag_ref)))]
    first = pl.multiple_of(lax.rem(5 - sp, 3) * shard_len, LANES)

    def chunk_copies(layer, k):
        rows = pl.ds(k * rows_per, rows_per)
        return [
            pltpu.make_async_copy(v_hbm.at[layer, :, rows, :], v_ref.at[layer, :, rows, :], chunk_sem.at[layer, k, 0]),
            pltpu.make_async_copy(z_hbm.at[layer, :, rows, :], z_ref.at[layer, :, rows, :], chunk_sem.at[layer, k, 1]),
            pltpu.make_async_copy(h_hbm.at[layer, :, rows, pl.ds(first, shard_len + LANES)], h_ref.at[layer, :, rows, :],
                                  chunk_sem.at[layer, k, 2]),
        ]

    def weight_copy(layer, n):
        src, dst = ((win_hbm, win), (wout_hbm, wout), (wup_hbm, wup), (wdown_hbm, wdown))[n]
        return pltpu.make_async_copy(src.at[layer], dst.at[layer], w_sem.at[layer, n])

    for copy in smalls:
        copy.start()
    for layer in range(LAYERS):
        for k in range(CHUNKS):
            for copy in chunk_copies(layer, k):
                copy.start()
        for n in range(4):
            weight_copy(layer, n).start()

    lane8 = lax.broadcasted_iota(jnp.int32, (8, LANES), 1)
    lane16 = lax.broadcasted_iota(jnp.int32, (16, LANES), 1)
    flip = [lax.rem(a - lane8 + 2 * LANES, LANES) for a in range(2)]

    def conv_group(cache, layer, which, row):
        accs = [[[None] * SEQ for _ in range(STEPS)] for _ in range(2)]

        def flipped(u, t):
            x = h_ref[layer, which, pl.ds(row + 8 * u, 8), LANES * t:LANES * (t + 1)]
            return [jnp.take_along_axis(x, flip[a], axis=1) for a in range(2)]

        def values(b, m):
            return cache[layer, b, pl.ds(row, 16), LANES * m:LANES * (m + 1)]

        zero = jnp.zeros((16, LANES), jnp.bfloat16)
        cur = [flipped(u, tiles) for u in range(2)]
        val = [values(b, 0) for b in range(SEQ)]
        rot = [pltpu.roll(val[b], LANES - 2, 1) for b in range(SEQ)]
        for b in range(SEQ):
            edge = jnp.where(lane16 >= LANES - 2, rot[b], zero).astype(jnp.float32)
            for u in range(2):
                for a in range(2):
                    accs[u][a + 2][b] = cur[u][a] * edge[8 * u:8 * u + 8]
        for m in range(tiles):
            nxt = [flipped(u, tiles - 1 - m) for u in range(2)]
            last = m == tiles - 1
            val_n = [None if last else values(b, m + 1) for b in range(SEQ)]
            rot_n = [zero if last else pltpu.roll(val_n[b], LANES - 2, 1) for b in range(SEQ)]
            here = [val[b].astype(jnp.float32) for b in range(SEQ)]
            ahead = [jnp.where(lane16 < LANES - 2, rot[b], rot_n[b]).astype(jnp.float32) for b in range(SEQ)]
            for u in range(2):
                for a in range(2):
                    taps = jnp.where(lane8 <= a, cur[u][a], nxt[u][a])
                    for b in range(SEQ):
                        p0 = taps * here[b][8 * u:8 * u + 8]
                        p2 = taps * ahead[b][8 * u:8 * u + 8]
                        accs[u][a][b] = p0 if m == 0 else accs[u][a][b] + p0
                        accs[u][a + 2][b] = accs[u][a + 2][b] + p2
            cur, val, rot = nxt, val_n, rot_n
        for u in range(2):
            for j in range(STEPS):
                for b in range(SEQ):
                    n = SEQ * j + b
                    acc[which, pl.ds(row + 8 * u, 8), LANES * n:LANES * (n + 1)] = accs[u][j][b]

    def conv(layer, k0, k1):
        def chunk(k, _):
            for copy in chunk_copies(layer, k):
                copy.wait()

            def group(g, _):
                row = pl.multiple_of(k * rows_per + g * 16, 16)
                conv_group(v_ref, layer, 0, row)
                conv_group(z_ref, layer, 1, row)
                return 0

            lax.fori_loop(0, rows_per // 16, group, 0)
            return 0

        lax.fori_loop(k0, k1, chunk, 0)

    lane_c = lax.broadcasted_iota(jnp.int32, (chan, LANES), 1)

    def hist_copies(layer):
        return [pltpu.make_async_remote_copy(hx.at[layer, sp], hx.at[layer, sp], hsend.at[layer, d], hrecv.at[layer, d],
                                             device_id=sp_peers[d], device_id_type=MESH) for d in (1, 0, 2)]

    def send_hist(layer):
        total = jnp.zeros((chan, LANES), jnp.float32)
        for which in range(2):
            for n in range(ROWS):
                part = jnp.sum(acc[which, :, LANES * n:LANES * (n + 1)], axis=1, keepdims=True)
                total = jnp.where(lane_c == which * ROWS + n, part, total)
        hx[layer, sp] = jnp.transpose(total)[:2 * ROWS]
        for copy in hist_copies(layer):
            copy.start()

    def sum_hist(layer):
        for copy in hist_copies(layer):
            copy.wait_recv()
        return ((hx[layer, 0] + hx[layer, 1]) + hx[layer, 2]) + hx[layer, 3]

    def sum_copies(n):
        return [pltpu.make_async_remote_copy(ar.at[n, tp], ar.at[n, tp], asend.at[n, d], arecv.at[n, d],
                                             device_id=peers[d], device_id_type=MESH) for d in (1, 0, 2)]

    def send_sum(n, part):
        ar[n, tp] = part
        for copy in sum_copies(n):
            copy.start()

    def take_sum(n):
        for copy in sum_copies(n):
            copy.wait_recv()
        return ((ar[n, 0] + ar[n, 1]) + ar[n, 2]) + ar[n, 3]

    row_c = lax.broadcasted_iota(jnp.int32, (ROWS, chan), 0)

    def project(layer, hidden):
        normed = layer_norm(hidden).astype(jnp.bfloat16)
        mixed = []
        for g in range(3):
            p = lax.dot_general(normed, win[layer, g], (((1,), (1,)), ((), ())), preferred_element_type=jnp.float32)
            p = (p + bin_ref[g, layer][None]).astype(jnp.bfloat16).astype(jnp.float32)
            for b in range(SEQ):
                pair = st_ref[layer, b, g].astype(jnp.float32)
                st8[b:b + 1, :] = pair[0:1]
                st8[SEQ + b:SEQ + b + 1, :] = pair[1:2]
            held = st8[...]
            prev1 = jnp.where(row_c < SEQ, pltpu.roll(held, ROWS - SEQ, 0), pltpu.roll(p, SEQ, 0))
            prev2 = jnp.where(row_c < 2 * SEQ, held, pltpu.roll(p, 2 * SEQ, 0))
            mixed.append(tap_ref[0, g, layer][None] * p + tap_ref[1, g, layer][None] * prev1 + tap_ref[2, g, layer][None] * prev2)
            for b in range(SEQ):
                for slot in range(2):
                    r = SEQ * (STEPS - 2 + slot) + b
                    st_out[layer, b, g, slot:slot + 1, :] = p[r:r + 1].astype(jnp.bfloat16)
        return mixed

    def recent(layer, which, rows_f):
        total = (lag[layer][which][0:1] + skip_ref[layer, which][None]) * rows_f
        for back in range(1, STEPS):
            shifted = jnp.where(row_c < SEQ * back, 0.0, pltpu.roll(rows_f, SEQ * back, 0))
            total = total + lag[layer][which][back:back + 1] * shifted
        return total

    def mixer(layer, mixed, hist):
        value = mixed[2].astype(jnp.bfloat16).astype(jnp.float32)
        long_one = hist[:ROWS] + recent(layer, 0, value)
        z_rows = (mixed[0] * long_one).astype(jnp.bfloat16).astype(jnp.float32)
        long_two = hist[ROWS:] + recent(layer, 1, z_rows)
        y_rows = (mixed[1] * long_two).astype(jnp.bfloat16)
        return value, z_rows, jnp.dot(y_rows, wout[layer], preferred_element_type=jnp.float32)

    def mlp(layer, hidden):
        up = jnp.dot(layer_norm(hidden).astype(jnp.bfloat16), wup[layer], preferred_element_type=jnp.float32)
        return jnp.dot(jax.nn.gelu(up).astype(jnp.bfloat16), wdown[layer], preferred_element_type=jnp.float32)

    def put_rows(layer, value, z_rows):
        for n, rows_f in enumerate((value, z_rows)):
            for b in range(SEQ):
                for j in range(STEPS):
                    r = SEQ * j + b
                    at = STEPS * (SEQ * n + b) + j
                    newrow[at:at + 1, 0:chan] = rows_f[r:r + 1]
        turned = jnp.transpose(newrow[...])[:chan]

        @pl.when(sp == 3)
        def _():
            for n, cache in enumerate((v_ref, z_ref)):
                for b in range(SEQ):
                    at = STEPS * (SEQ * n + b)
                    moved = turned if at == 0 else pltpu.roll(turned, LANES - at, 1)
                    cache[layer, b, :, 0:LANES] = jnp.where(lane_c < STEPS, moved, 0.0).astype(jnp.bfloat16)

    newrow[...] = jnp.zeros_like(newrow)
    st8[...] = jnp.zeros_like(st8)
    for copy in smalls:
        copy.wait()
    lag = [[jnp.transpose(lag_ref[layer, which])[:8] for which in range(2)] for layer in range(LAYERS)]
    hidden = jnp.concatenate([e_ref[j].astype(jnp.float32) for j in range(STEPS)], axis=0)

    conv(0, 0, CHUNKS)
    pl.semaphore_wait(barrier, 6)
    send_hist(0)
    weight_copy(0, 0).wait()
    mixed = project(0, hidden)
    weight_copy(0, 1).wait()
    value, z_rows, part = mixer(0, mixed, sum_hist(0))
    send_sum(0, part)
    conv(1, 0, CHUNKS // 2)
    weight_copy(0, 2).wait()
    weight_copy(0, 3).wait()
    hidden = hidden + take_sum(0) + bout_ref[0:1]
    send_sum(1, mlp(0, hidden))
    conv(1, CHUNKS // 2, CHUNKS)
    send_hist(1)
    put_rows(0, value, z_rows)
    weight_copy(1, 0).wait()
    hidden = hidden + take_sum(1)
    mixed = project(1, hidden)
    weight_copy(1, 1).wait()
    value, z_rows, part = mixer(1, mixed, sum_hist(1))
    send_sum(2, part)
    put_rows(1, value, z_rows)
    weight_copy(1, 2).wait()
    weight_copy(1, 3).wait()
    hidden = hidden + take_sum(2) + bout_ref[1:2]
    send_sum(3, mlp(1, hidden))
    hidden = hidden + take_sum(3)
    for j in range(STEPS):
        hid_out[j] = hidden[SEQ * j:SEQ * j + SEQ]
    for layer in range(LAYERS):
        for copy in hist_copies(layer):
            copy.wait_send()
    for n in range(4):
        for copy in sum_copies(n):
            copy.wait_send()


def solution(mesh):
    def device_fn(step_emb, v_cache, z_cache, short_state, w_in, b_in, short_taps, long_filt, skip_gain, w_out, b_out, w_up, w_down):
        chan = v_cache.shape[3]
        shard_len = v_cache.shape[2]
        model = step_emb.shape[2]
        args = (
            step_emb,
            jnp.swapaxes(v_cache, 2, 3),
            jnp.swapaxes(z_cache, 2, 3),
            jnp.transpose(short_state, (0, 1, 3, 2, 4)),
            jnp.transpose(w_in, (0, 2, 3, 1)),
            jnp.transpose(b_in, (1, 0, 2)),
            jnp.transpose(short_taps, (1, 2, 0, 3)),
            jnp.swapaxes(long_filt, 2, 3),
            skip_gain,
            w_out,
            b_out,
            w_up,
            w_down,
        )
        f32, bf16 = jnp.float32, jnp.bfloat16
        dma = pltpu.SemaphoreType.DMA
        hid, v_out, z_out, st_out = pl.pallas_call(
            kernel,
            out_shape=(
                jax.ShapeDtypeStruct(step_emb.shape, f32),
                pltpu.VMEM(args[1].shape, bf16),
                pltpu.VMEM(args[2].shape, bf16),
                jax.ShapeDtypeStruct(args[3].shape, bf16),
            ),
            in_specs=[pl.BlockSpec(memory_space=pl.ANY)] * 13,
            out_specs=[pl.BlockSpec(memory_space=pltpu.VMEM)] * 4,
            scratch_shapes=[
                pltpu.VMEM(step_emb.shape, bf16),
                pltpu.VMEM(args[3].shape, bf16),
                pltpu.VMEM(args[4].shape, bf16),
                pltpu.VMEM(args[5].shape, f32),
                pltpu.VMEM(args[6].shape, f32),
                pltpu.VMEM((LAYERS, 2, chan, shard_len + LANES), f32),
                pltpu.VMEM((LAYERS, 2, chan, LANES), f32),
                pltpu.VMEM(skip_gain.shape, f32),
                pltpu.VMEM(w_out.shape, bf16),
                pltpu.VMEM(b_out.shape, f32),
                pltpu.VMEM(w_up.shape, bf16),
                pltpu.VMEM(w_down.shape, bf16),
                pltpu.VMEM((2, chan, ROWS * LANES), f32),
                pltpu.VMEM((ROWS, chan), f32),
                pltpu.VMEM((LANES, 2 * LANES), f32),
                pltpu.VMEM((LAYERS, 4, 2 * ROWS, chan), f32),
                pltpu.VMEM((4, 4, ROWS, model), f32),
                dma((7,)),
                dma((LAYERS, CHUNKS, 3)),
                dma((LAYERS, 4)),
                dma((LAYERS, 3)),
                dma((LAYERS, 3)),
                dma((4, 3)),
                dma((4, 3)),
                dma,
            ],
            compiler_params=pltpu.CompilerParams(collective_id=0, has_side_effects=True, vmem_limit_bytes=40 * 1024 * 1024),
            name="decode",
        )(*args)
        return (hid, jnp.swapaxes(v_out, 2, 3), jnp.swapaxes(z_out, 2, 3), jnp.transpose(st_out, (0, 1, 3, 2, 4)))

    specs_in = (
        P(None, "dp", None),
        P(None, "dp", "sp", "tp"),
        P(None, "dp", "sp", "tp"),
        P(None, "dp", None, None, "tp"),
        P(None, None, None, "tp"),
        P(None, None, "tp"),
        P(None, None, None, "tp"),
        P(None, None, None, "tp"),
        P(None, None, "tp"),
        P(None, "tp", None),
        P(None, None),
        P(None, None, "tp"),
        P(None, "tp", None),
    )
    specs_out = (
        P(None, "dp", None),
        P(None, "dp", "sp", "tp"),
        P(None, "dp", "sp", "tp"),
        P(None, "dp", None, None, "tp"),
    )
    return jax.shard_map(device_fn, mesh=mesh, in_specs=specs_in, out_specs=specs_out, check_vma=False)
```

```python
import functools

import jax
import jax.numpy as jnp
from jax import lax
from jax.experimental import pallas as pl
from jax.experimental.pallas import tpu as pltpu
from jax.sharding import PartitionSpec as P

STEPS = 4
LAYERS = 2
SEQ = 2
ROWS = STEPS * SEQ
LANES = 128
CHUNKS = 12
SPLIT = 7
MESH = pl.DeviceIdType.MESH


def layer_norm(rows_in):
    mean_val = jnp.mean(rows_in, axis=-1, keepdims=True)
    centered = rows_in - mean_val
    var_val = jnp.mean(centered * centered, axis=-1, keepdims=True)
    return centered * lax.rsqrt(var_val + 1e-5)


def kernel(e_hbm, v_hbm, z_hbm, st_hbm, win_hbm, bin_hbm, tap_hbm, h_hbm, skip_hbm, wout_hbm, bout_hbm, wup_hbm, wdown_hbm,
           hid_out, v_ref, z_ref, st_out,
           e_ref, st_ref, win, bin_ref, tap_ref, h_ref, lag_ref, skip_ref, wout, bout_ref, wup, wdown,
           acc, prow, rrow, newrow, hx, ar, xb, fin,
           small_sem, chunk_sem, w_sem, hsend, hrecv, asend, arecv, xsem, fsem):
    tp = lax.axis_index("tp")
    sp = lax.axis_index("sp")
    core = lax.rem(sp, 2)
    chan, shard_len = v_hbm.shape[2], v_hbm.shape[3]
    model = e_hbm.shape[2]
    tiles = shard_len // LANES
    rows_per = chan // CHUNKS
    half = lax.div(tp, 2)
    near = tp + 1 - 2 * lax.rem(tp, 2)
    peers = [{"tp": 3 - 3 * half}, {"tp": 2 - half}, {"tp": near}]
    across = lax.rem(sp + 2, 4)
    sp_peers = [(across, core), (across + 1 - 2 * core, 1 - core), (sp + 1 - 2 * core, 1 - core)]
    partner = {"sp": sp + 1 - 2 * core}

    barrier = pltpu.get_barrier_semaphore()
    for peer in peers + [{"sp": other} for other, _ in sp_peers]:
        pl.semaphore_signal(barrier, inc=1, device_id=peer, device_id_type=MESH)

    smalls = [pltpu.make_async_copy(src, dst, small_sem.at[n]) for n, (src, dst) in enumerate((
        (e_hbm, e_ref), (st_hbm, st_ref), (bin_hbm, bin_ref), (tap_hbm, tap_ref), (skip_hbm, skip_ref), (bout_hbm, bout_ref),
        (h_hbm.at[:, :, :, pl.ds(0, LANES)], lag_ref)))]
    first = pl.multiple_of(lax.rem(5 - sp, 3) * shard_len, LANES)

    def chunk_copies(layer, k):
        rows = pl.ds(k * rows_per if isinstance(k, int) else pl.multiple_of(k * rows_per, rows_per), rows_per)
        return [
            pltpu.make_async_copy(v_hbm.at[layer, :, rows, :], v_ref.at[layer, :, rows, :], chunk_sem.at[layer, k, 0]),
            pltpu.make_async_copy(z_hbm.at[layer, :, rows, :], z_ref.at[layer, :, rows, :], chunk_sem.at[layer, k, 1]),
            pltpu.make_async_copy(h_hbm.at[layer, :, rows, pl.ds(first, shard_len + LANES)], h_ref.at[layer, :, rows, :],
                                  chunk_sem.at[layer, k, 2]),
        ]

    def weight_copy(layer, n):
        src, dst = ((win_hbm, win), (wout_hbm, wout), (wup_hbm, wup), (wdown_hbm, wdown))[n]
        return pltpu.make_async_copy(src.at[layer], dst.at[layer], w_sem.at[layer, n])

    for layer in range(LAYERS):
        for k in range(CHUNKS):
            for copy in chunk_copies(layer, k):
                copy.start()
        if layer == 0:
            for copy in smalls:
                copy.start()
        for n in range(4):
            weight_copy(layer, n).start()

    lane8 = lax.broadcasted_iota(jnp.int32, (8, LANES), 1)
    lane16 = lax.broadcasted_iota(jnp.int32, (16, LANES), 1)
    flip = [lax.rem(a - lane8 + 2 * LANES, LANES) for a in range(2)]

    def conv_group(cache, layer, which, row):
        accs = [[[None] * SEQ for _ in range(STEPS)] for _ in range(2)]

        def flipped(u, t):
            x = h_ref[layer, which, pl.ds(row + 8 * u, 8), LANES * t:LANES * (t + 1)]
            return [jnp.take_along_axis(x, flip[a], axis=1) for a in range(2)]

        def values(b, m):
            return cache[layer, b, pl.ds(row, 16), LANES * m:LANES * (m + 1)]

        zero = jnp.zeros((16, LANES), jnp.bfloat16)
        cur = [flipped(u, tiles) for u in range(2)]
        val = [values(b, 0) for b in range(SEQ)]
        rot = [pltpu.roll(val[b], LANES - 2, 1) for b in range(SEQ)]
        for b in range(SEQ):
            edge = jnp.where(lane16 >= LANES - 2, rot[b], zero).astype(jnp.float32)
            for u in range(2):
                for a in range(2):
                    accs[u][a + 2][b] = cur[u][a] * edge[8 * u:8 * u + 8]
        for m in range(tiles):
            nxt = [flipped(u, tiles - 1 - m) for u in range(2)]
            last = m == tiles - 1
            val_n = [None if last else values(b, m + 1) for b in range(SEQ)]
            rot_n = [zero if last else pltpu.roll(val_n[b], LANES - 2, 1) for b in range(SEQ)]
            here = [val[b].astype(jnp.float32) for b in range(SEQ)]
            ahead = [jnp.where(lane16 < LANES - 2, rot[b], rot_n[b]).astype(jnp.float32) for b in range(SEQ)]
            for u in range(2):
                for a in range(2):
                    taps = jnp.where(lane8 <= a, cur[u][a], nxt[u][a])
                    for b in range(SEQ):
                        p0 = taps * here[b][8 * u:8 * u + 8]
                        p2 = taps * ahead[b][8 * u:8 * u + 8]
                        accs[u][a][b] = p0 if m == 0 else accs[u][a][b] + p0
                        accs[u][a + 2][b] = accs[u][a + 2][b] + p2
            cur, val, rot = nxt, val_n, rot_n
        for u in range(2):
            for j in range(STEPS):
                for b in range(SEQ):
                    n = SEQ * j + b
                    acc[which, pl.ds(row + 8 * u, 8), LANES * n:LANES * (n + 1)] = accs[u][j][b]

    def conv(layer, k0, k1):
        def chunk(k, _):
            for copy in chunk_copies(layer, k):
                copy.wait()

            def group(g, _):
                row = pl.multiple_of(k * rows_per + g * 16, 16)
                conv_group(v_ref, layer, 0, row)
                conv_group(z_ref, layer, 1, row)
                return 0

            lax.fori_loop(0, rows_per // 16, group, 0)
            return 0

        lax.fori_loop(k0, k1, chunk, 0)

    lane_c = lax.broadcasted_iota(jnp.int32, (chan, LANES), 1)

    def hist_copies(layer):
        return [pltpu.make_async_remote_copy(hx.at[layer, sp, seq], hx.at[layer, sp, seq], hsend.at[layer, d], hrecv.at[layer, sp],
                                             device_id={"sp": other}, device_id_type=MESH)
                for d, (other, seq) in enumerate(sp_peers)]

    def send_hist(layer):
        total = jnp.zeros((chan, LANES), jnp.float32)
        for which in range(2):
            for j in range(STEPS):
                for b in range(SEQ):
                    n = SEQ * j + b
                    part = jnp.sum(acc[which, :, LANES * n:LANES * (n + 1)], axis=1, keepdims=True)
                    total = jnp.where(lane_c == (2 * b + which) * STEPS + j, part, total)
        turned = jnp.transpose(total)
        for b in range(SEQ):
            hx[layer, sp, b] = turned[2 * STEPS * b:2 * STEPS * (b + 1)]

        @pl.when(sp != 3)
        def _():
            for copy in hist_copies(layer):
                copy.start()

    def sum_hist(layer):
        for src in range(3):
            @pl.when(sp != src)
            def _():
                pltpu.make_async_remote_copy(hx.at[layer, src, core], hx.at[layer, src, core], hsend.at[layer, 0], hrecv.at[layer, src],
                                             device_id=partner, device_id_type=MESH).wait_recv()
        return (hx[layer, 0, core] + hx[layer, 1, core]) + hx[layer, 2, core]

    def sum_copies(n):
        return [pltpu.make_async_remote_copy(ar.at[n, tp], ar.at[n, tp], asend.at[n, d], arecv.at[n, tp],
                                             device_id=peers[d], device_id_type=MESH) for d in range(3)]

    def send_sum(n, part):
        ar[n, tp] = part
        for copy in sum_copies(n):
            copy.start()

    def take_sum(n):
        for d in (1, 2, 3):
            src = lax.rem(tp + d, 4)
            pltpu.make_async_remote_copy(ar.at[n, src], ar.at[n, src], asend.at[n, 0], arecv.at[n, src],
                                         device_id=peers[0], device_id_type=MESH).wait_recv()
        return ((ar[n, 0] + ar[n, 1]) + ar[n, 2]) + ar[n, 3]

    def swap_copy(layer):
        return pltpu.make_async_remote_copy(xb.at[layer, core], xb.at[layer, core], xsem.at[layer, 0], xsem.at[layer, 1],
                                            device_id=partner, device_id_type=MESH)

    def project(layer, hidden):
        normed = layer_norm(hidden).astype(jnp.bfloat16)
        mixed = []
        for g in range(3):
            p = lax.dot_general(normed, win[layer, g], (((1,), (1,)), ((), ())), preferred_element_type=jnp.float32)
            p = (p + bin_ref[g, layer][None]).astype(jnp.bfloat16).astype(jnp.float32)
            prow[layer, g, 0:2, :] = st_ref[layer, core, g].astype(jnp.float32)
            prow[layer, g, 2:2 + STEPS, :] = p
            mixed.append(tap_ref[0, g, layer][None] * p + tap_ref[1, g, layer][None] * prow[layer, g, 1:1 + STEPS, :]
                         + tap_ref[2, g, layer][None] * prow[layer, g, 0:STEPS, :])
        return mixed

    def recent(layer, which, rows_f):
        rrow[layer, which, STEPS - 1:2 * STEPS - 1, :] = rows_f
        total = (lag[layer][which][0:1] + skip_ref[layer, which][None]) * rows_f
        for back in range(1, STEPS):
            total = total + lag[layer][which][back:back + 1] * rrow[layer, which, STEPS - 1 - back:2 * STEPS - 1 - back, :]
        return total

    def mixer(layer, mixed, hist):
        value = mixed[2].astype(jnp.bfloat16).astype(jnp.float32)
        long_one = hist[:STEPS] + recent(layer, 0, value)
        z_rows = (mixed[0] * long_one).astype(jnp.bfloat16).astype(jnp.float32)
        long_two = hist[STEPS:] + recent(layer, 1, z_rows)
        y_rows = (mixed[1] * long_two).astype(jnp.bfloat16)
        send_sum(2 * layer, jnp.dot(y_rows, wout[layer], preferred_element_type=jnp.float32))
        for g in range(3):
            xb[layer, core, 2 * g:2 * g + 2, :] = prow[layer, g, STEPS:STEPS + 2, :]
        xb[layer, core, 6:8, :] = jnp.zeros((2, chan), jnp.float32)
        xb[layer, core, 8:8 + STEPS, :] = value
        xb[layer, core, 8 + STEPS:8 + 2 * STEPS, :] = z_rows
        swap_copy(layer).start()

    def mlp(layer, hidden):
        up = jnp.dot(layer_norm(hidden).astype(jnp.bfloat16), wup[layer], preferred_element_type=jnp.float32)
        return jnp.dot(jax.nn.gelu(up).astype(jnp.bfloat16), wdown[layer], preferred_element_type=jnp.float32)

    def put_rows(layer):
        swap_copy(layer).wait_recv()
        for b in range(SEQ):
            newrow[2 * STEPS * b:2 * STEPS * (b + 1), 0:chan] = xb[layer, b, 8:16, :]
            for g in range(3):
                st_out[layer, b, g] = xb[layer, b, 2 * g:2 * g + 2, :].astype(jnp.bfloat16)
        turned = jnp.transpose(newrow[...])[:chan]

        @pl.when(sp == 3)
        def _():
            for b in range(SEQ):
                for n, cache in enumerate((v_ref, z_ref)):
                    at = STEPS * (2 * b + n)
                    moved = turned if at == 0 else pltpu.roll(turned, LANES - at, 1)
                    cache[layer, b, :, 0:LANES] = jnp.where(lane_c < STEPS, moved, 0.0).astype(jnp.bfloat16)

    conv(0, 0, CHUNKS)
    pl.semaphore_wait(barrier, 6)
    send_hist(0)
    newrow[...] = jnp.zeros_like(newrow)
    rrow[...] = jnp.zeros_like(rrow)
    for copy in smalls:
        copy.wait()
    hidden = jnp.where(core == 0, jnp.concatenate([e_ref[j].astype(jnp.float32)[0:1] for j in range(STEPS)], axis=0),
                       jnp.concatenate([e_ref[j].astype(jnp.float32)[1:2] for j in range(STEPS)], axis=0))
    lag = [[jnp.transpose(lag_ref[layer, which])[:8] for which in range(2)] for layer in range(LAYERS)]
    weight_copy(0, 0).wait()
    mixed = project(0, hidden)
    weight_copy(0, 1).wait()
    mixer(0, mixed, sum_hist(0))
    conv(1, 0, SPLIT)
    weight_copy(0, 2).wait()
    weight_copy(0, 3).wait()
    hidden = hidden + take_sum(0) + bout_ref[0:1]
    send_sum(1, mlp(0, hidden))
    conv(1, SPLIT, CHUNKS)
    send_hist(1)
    weight_copy(1, 0).wait()
    hidden = hidden + take_sum(1)
    mixed = project(1, hidden)
    weight_copy(1, 1).wait()
    mixer(1, mixed, sum_hist(1))
    put_rows(0)
    weight_copy(1, 2).wait()
    weight_copy(1, 3).wait()
    hidden = hidden + take_sum(2) + bout_ref[1:2]
    send_sum(3, mlp(1, hidden))
    put_rows(1)
    hidden = hidden + take_sum(3)
    fin[core] = hidden
    last = pltpu.make_async_remote_copy(fin.at[core], fin.at[core], fsem.at[0], fsem.at[1], device_id=partner, device_id_type=MESH)
    last.start()
    for layer in range(LAYERS):
        swap_copy(layer).wait_send()

        @pl.when(sp != 3)
        def _():
            for copy in hist_copies(layer):
                copy.wait_send()
    for n in range(4):
        for copy in sum_copies(n):
            copy.wait_send()
    last.wait()
    for b in range(SEQ):
        for j in range(STEPS):
            hid_out[j, b:b + 1, :] = fin[b, j:j + 1, :]


def emit(hid, v, z, st, hid_o, v_o, z_o, st_o, sem):
    copies = []
    for layer in range(LAYERS):
        for b in range(SEQ):
            copies += [(v.at[layer, b], v_o.at[layer, b]), (z.at[layer, b], z_o.at[layer, b])]
    copies += [(hid, hid_o), (st, st_o)]
    copies = [pltpu.make_async_copy(src, dst, sem.at[n]) for n, (src, dst) in enumerate(copies)]
    for copy in copies:
        copy.start()
    for copy in copies:
        copy.wait()


def solution(mesh):
    def device_fn(step_emb, v_cache, z_cache, short_state, w_in, b_in, short_taps, long_filt, skip_gain, w_out, b_out, w_up, w_down):
        chan = v_cache.shape[3]
        shard_len = v_cache.shape[2]
        model = step_emb.shape[2]
        args = (
            step_emb,
            jnp.swapaxes(v_cache, 2, 3),
            jnp.swapaxes(z_cache, 2, 3),
            jnp.transpose(short_state, (0, 1, 3, 2, 4)),
            jnp.transpose(w_in, (0, 2, 3, 1)),
            jnp.transpose(b_in, (1, 0, 2)),
            jnp.transpose(short_taps, (1, 2, 0, 3)),
            jnp.swapaxes(long_filt, 2, 3),
            skip_gain,
            w_out,
            b_out,
            w_up,
            w_down,
        )
        args = tuple(pltpu.with_memory_space_constraint(arg, pltpu.HBM) for arg in args)
        f32, bf16 = jnp.float32, jnp.bfloat16
        dma = pltpu.SemaphoreType.DMA
        hid, v_out, z_out, st_out = pl.pallas_call(
            kernel,
            out_shape=(
                jax.ShapeDtypeStruct(step_emb.shape, f32),
                pltpu.VMEM(args[1].shape, bf16),
                pltpu.VMEM(args[2].shape, bf16),
                jax.ShapeDtypeStruct(args[3].shape, bf16),
            ),
            in_specs=[pl.BlockSpec(memory_space=pltpu.HBM)] * 13,
            out_specs=[pl.BlockSpec(memory_space=pltpu.VMEM)] * 4,
            scratch_shapes=[
                pltpu.VMEM(step_emb.shape, bf16),
                pltpu.VMEM(args[3].shape, bf16),
                pltpu.VMEM(args[4].shape, bf16),
                pltpu.VMEM(args[5].shape, f32),
                pltpu.VMEM(args[6].shape, f32),
                pltpu.VMEM((LAYERS, 2, chan, shard_len + LANES), f32),
                pltpu.VMEM((LAYERS, 2, chan, LANES), f32),
                pltpu.VMEM(skip_gain.shape, f32),
                pltpu.VMEM(w_out.shape, bf16),
                pltpu.VMEM(b_out.shape, f32),
                pltpu.VMEM(w_up.shape, bf16),
                pltpu.VMEM(w_down.shape, bf16),
                pltpu.VMEM((2, chan, ROWS * LANES), f32),
                pltpu.VMEM((LAYERS, 3, 8, chan), f32),
                pltpu.VMEM((LAYERS, 2, 8, chan), f32),
                pltpu.VMEM((LANES, 2 * LANES), f32),
                pltpu.VMEM((LAYERS, 4, SEQ, 2 * STEPS, chan), f32),
                pltpu.VMEM((4, 4, STEPS, model), f32),
                pltpu.VMEM((LAYERS, SEQ, 16, chan), f32),
                pltpu.VMEM((SEQ, STEPS, model), f32),
                dma((7,)),
                dma((LAYERS, CHUNKS, 3)),
                dma((LAYERS, 4)),
                dma((LAYERS, 3)),
                dma((LAYERS, 4)),
                dma((4, 3)),
                dma((4, 4)),
                dma((LAYERS, 2)),
                dma((2,)),
            ],
            compiler_params=pltpu.CompilerParams(collective_id=0, has_side_effects=True, vmem_limit_bytes=40 * 1024 * 1024),
            name="decode",
        )(*args)
        hid, v_out, z_out, st_out = pl.pallas_call(
            emit,
            out_shape=(
                jax.ShapeDtypeStruct(hid.shape, f32),
                jax.ShapeDtypeStruct(v_out.shape, bf16),
                jax.ShapeDtypeStruct(z_out.shape, bf16),
                jax.ShapeDtypeStruct(st_out.shape, bf16),
            ),
            in_specs=[pl.BlockSpec(memory_space=pltpu.VMEM)] * 4,
            out_specs=[pl.BlockSpec(memory_space=pltpu.HBM)] * 4,
            scratch_shapes=[dma((4 * LAYERS + 2,))],
            compiler_params=pltpu.CompilerParams(vmem_limit_bytes=1024 * 1024),
            name="emit",
        )(hid, v_out, z_out, st_out)
        return (hid, jnp.swapaxes(v_out, 2, 3), jnp.swapaxes(z_out, 2, 3), jnp.transpose(st_out, (0, 1, 3, 2, 4)))

    specs_in = (
        P(None, "dp", None),
        P(None, "dp", "sp", "tp"),
        P(None, "dp", "sp", "tp"),
        P(None, "dp", None, None, "tp"),
        P(None, None, None, "tp"),
        P(None, None, "tp"),
        P(None, None, None, "tp"),
        P(None, None, None, "tp"),
        P(None, None, "tp"),
        P(None, "tp", None),
        P(None, None),
        P(None, None, "tp"),
        P(None, "tp", None),
    )
    specs_out = (
        P(None, "dp", None),
        P(None, "dp", "sp", "tp"),
        P(None, "dp", "sp", "tp"),
        P(None, "dp", None, None, "tp"),
    )
    return jax.shard_map(device_fn, mesh=mesh, in_specs=specs_in, out_specs=specs_out, check_vma=False)
```

```python
import functools

import jax
import jax.numpy as jnp
from jax import lax
from jax.experimental import pallas as pl
from jax.experimental.pallas import tpu as pltpu
from jax.sharding import PartitionSpec as P

STEPS = 4
LAYERS = 2
SEQ = 2
ROWS = STEPS * SEQ
LANES = 128
CHUNKS = 12
SPLIT = 7
MESH = pl.DeviceIdType.MESH


def layer_norm(rows_in):
    mean_val = jnp.mean(rows_in, axis=-1, keepdims=True)
    centered = rows_in - mean_val
    var_val = jnp.mean(centered * centered, axis=-1, keepdims=True)
    return centered * lax.rsqrt(var_val + 1e-5)


def kernel(e_hbm, v_hbm, z_hbm, st_hbm, win_hbm, bin_hbm, tap_hbm, h_hbm, skip_hbm, wout_hbm, bout_hbm, wup_hbm, wdown_hbm,
           hid_out, v_ref, z_ref, st_out,
           e_ref, st_ref, win, bin_ref, tap_ref, h_ref, lag_ref, skip_ref, wout, bout_ref, wup, wdown,
           acc, total, lag, prow, rrow, newrow, hx, ar, xb, fin,
           small_sem, chunk_sem, w_sem, hsend, hrecv, asend, arecv, xsend, xrecv, fsend, frecv):
    tp = lax.axis_index("tp")
    sp = lax.axis_index("sp")
    own = lax.div(sp, 2)
    carries = lax.rem(sp, 2) == 1
    has_rows = sp != 3
    chan, shard_len = v_hbm.shape[2], v_hbm.shape[3]
    model = e_hbm.shape[2]
    tiles = shard_len // LANES
    rows_per = chan // CHUNKS
    half = lax.div(tp, 2)
    near = tp + 1 - 2 * lax.rem(tp, 2)
    peers = [{"tp": 3 - 3 * half}, {"tp": 2 - half}, {"tp": near}]
    block_peers = [{"sp": lax.rem(sp + d, 4)} for d in (2, 3, 1)]

    barrier = pltpu.get_barrier_semaphore()
    for peer in block_peers:
        pl.semaphore_signal(barrier, inc=1, device_id=peer, device_id_type=MESH)

    @pl.when(carries)
    def _():
        for peer in peers:
            pl.semaphore_signal(barrier, inc=1, device_id=peer, device_id_type=MESH)

    smalls = [pltpu.make_async_copy(src, dst, small_sem.at[n]) for n, (src, dst) in enumerate((
        (e_hbm, e_ref), (st_hbm, st_ref), (bin_hbm, bin_ref), (tap_hbm, tap_ref), (skip_hbm, skip_ref), (bout_hbm, bout_ref),
        (h_hbm.at[:, :, :, pl.ds(0, LANES)], lag_ref)))]
    first = pl.multiple_of(lax.rem(5 - sp, 3) * shard_len, LANES)

    def chunk_copies(layer, k):
        rows = pl.ds(k * rows_per if isinstance(k, int) else pl.multiple_of(k * rows_per, rows_per), rows_per)
        return [
            pltpu.make_async_copy(v_hbm.at[layer, :, rows, :], v_ref.at[layer, :, rows, :], chunk_sem.at[layer, k, 0]),
            pltpu.make_async_copy(z_hbm.at[layer, :, rows, :], z_ref.at[layer, :, rows, :], chunk_sem.at[layer, k, 1]),
            pltpu.make_async_copy(h_hbm.at[layer, :, rows, pl.ds(first, shard_len + LANES)], h_ref.at[layer, :, rows, :],
                                  chunk_sem.at[layer, k, 2]),
        ]

    def weight_copy(layer, n):
        src, dst = ((win_hbm, win), (wout_hbm, wout), (wup_hbm, wup), (wdown_hbm, wdown))[n]
        return pltpu.make_async_copy(src.at[layer], dst.at[layer], w_sem.at[layer, n])

    for layer in range(LAYERS):
        for k in range(CHUNKS):
            for copy in chunk_copies(layer, k):
                copy.start()
        if layer == 0:
            for copy in smalls:
                copy.start()
        for n in range(4):
            weight_copy(layer, n).start()

    lane8 = lax.broadcasted_iota(jnp.int32, (8, LANES), 1)
    lane16 = lax.broadcasted_iota(jnp.int32, (16, LANES), 1)
    flip = [lax.rem(a - lane8 + 2 * LANES, LANES) for a in range(2)]

    def conv_group(cache, layer, which, row):
        accs = [[[None] * SEQ for _ in range(STEPS)] for _ in range(2)]

        def flipped(u, t):
            x = h_ref[layer, which, pl.ds(row + 8 * u, 8), LANES * t:LANES * (t + 1)]
            return [jnp.take_along_axis(x, flip[a], axis=1) for a in range(2)]

        def values(b, m):
            return cache[layer, b, pl.ds(row, 16), LANES * m:LANES * (m + 1)]

        zero = jnp.zeros((16, LANES), jnp.bfloat16)
        cur = [flipped(u, tiles) for u in range(2)]
        val = [values(b, 0) for b in range(SEQ)]
        rot = [pltpu.roll(val[b], LANES - 2, 1) for b in range(SEQ)]
        for b in range(SEQ):
            edge = jnp.where(lane16 >= LANES - 2, rot[b], zero).astype(jnp.float32)
            for u in range(2):
                for a in range(2):
                    accs[u][a + 2][b] = cur[u][a] * edge[8 * u:8 * u + 8]
        for m in range(tiles):
            nxt = [flipped(u, tiles - 1 - m) for u in range(2)]
            last = m == tiles - 1
            val_n = [None if last else values(b, m + 1) for b in range(SEQ)]
            rot_n = [zero if last else pltpu.roll(val_n[b], LANES - 2, 1) for b in range(SEQ)]
            here = [val[b].astype(jnp.float32) for b in range(SEQ)]
            ahead = [jnp.where(lane16 < LANES - 2, rot[b], rot_n[b]).astype(jnp.float32) for b in range(SEQ)]
            for u in range(2):
                for a in range(2):
                    taps = jnp.where(lane8 <= a, cur[u][a], nxt[u][a])
                    for b in range(SEQ):
                        p0 = taps * here[b][8 * u:8 * u + 8]
                        p2 = taps * ahead[b][8 * u:8 * u + 8]
                        accs[u][a][b] = p0 if m == 0 else accs[u][a][b] + p0
                        accs[u][a + 2][b] = accs[u][a + 2][b] + p2
            cur, val, rot = nxt, val_n, rot_n
        for u in range(2):
            for j in range(STEPS):
                for b in range(SEQ):
                    n = SEQ * j + b
                    acc[which, pl.ds(row + 8 * u, 8), LANES * n:LANES * (n + 1)] = accs[u][j][b]

    def close(row):
        out = jnp.zeros((16, LANES), jnp.float32)
        for which in range(2):
            for j in range(STEPS):
                for b in range(SEQ):
                    n = SEQ * j + b
                    part = jnp.sum(acc[which, pl.ds(row, 16), LANES * n:LANES * (n + 1)], axis=1, keepdims=True)
                    out = jnp.where(lane16 == (2 * b + which) * STEPS + j, part, out)
        total[pl.ds(row, 16), :] = out

    def conv(layer, k0, k1):
        def chunk(k, _):
            for copy in chunk_copies(layer, k):
                copy.wait()

            @pl.when(has_rows)
            def _():
                row = pl.multiple_of(k * 16, 16)
                conv_group(v_ref, layer, 0, row)
                conv_group(z_ref, layer, 1, row)

            return 0

        lax.fori_loop(k0, k1, chunk, 0)

    lane_c = lax.broadcasted_iota(jnp.int32, (chan, LANES), 1)

    def hist_copy(layer, seq):
        return pltpu.make_async_remote_copy(hx.at[layer, sp, seq], hx.at[layer, sp, seq], hsend.at[layer, seq], hrecv.at[layer, sp],
                                            device_id={"sp": 2 * seq + 1}, device_id_type=MESH)

    def send_hist(layer):
        @pl.when(has_rows)
        def _():
            for row in range(0, chan, 16):
                close(row)
            turned = jnp.transpose(total[...])
            for b in range(SEQ):
                hx[layer, sp, b] = turned[2 * STEPS * b:2 * STEPS * (b + 1)]
            hist_copy(layer, 1).start()

            @pl.when(sp != 1)
            def _():
                hist_copy(layer, 0).start()

    def sum_hist(layer):
        for src in range(3):
            @pl.when(sp != src)
            def _():
                pltpu.make_async_remote_copy(hx.at[layer, src, own], hx.at[layer, src, own], hsend.at[layer, 0], hrecv.at[layer, src],
                                             device_id=block_peers[0], device_id_type=MESH).wait_recv()
        return (hx[layer, 0, own] + hx[layer, 1, own]) + hx[layer, 2, own]

    def sum_copies(n):
        return [pltpu.make_async_remote_copy(ar.at[n, tp], ar.at[n, tp], asend.at[n, d], arecv.at[n, tp],
                                             device_id=peers[d], device_id_type=MESH) for d in range(3)]

    def send_sum(n, part):
        ar[n, tp] = part
        for copy in sum_copies(n):
            copy.start()

    def take_sum(n):
        for d in (1, 2, 3):
            src = lax.rem(tp + d, 4)
            pltpu.make_async_remote_copy(ar.at[n, src], ar.at[n, src], asend.at[n, 0], arecv.at[n, src],
                                         device_id=peers[0], device_id_type=MESH).wait_recv()
        return ((ar[n, 0] + ar[n, 1]) + ar[n, 2]) + ar[n, 3]

    def row_copy(layer, seq, d):
        return pltpu.make_async_remote_copy(xb.at[layer, seq], xb.at[layer, seq], xsend.at[layer, d], xrecv.at[layer, seq],
                                            device_id=block_peers[d], device_id_type=MESH)

    def row_copies(layer, seq):
        return [row_copy(layer, seq, d) for d in range(3)]

    def last_copy(seq, d):
        return pltpu.make_async_remote_copy(fin.at[seq], fin.at[seq], fsend.at[d], frecv.at[seq],
                                            device_id=block_peers[d], device_id_type=MESH)

    def last_copies(seq):
        return [last_copy(seq, d) for d in range(3)]

    def project(layer, hidden):
        normed = layer_norm(hidden).astype(jnp.bfloat16)
        mixed = []
        for g in range(3):
            p = lax.dot_general(normed, win[layer, g], (((1,), (1,)), ((), ())), preferred_element_type=jnp.float32)
            p = (p + bin_ref[g, layer][None]).astype(jnp.bfloat16).astype(jnp.float32)
            prow[layer, g, 0:2, :] = st_ref[layer, own, g].astype(jnp.float32)
            prow[layer, g, 2:2 + STEPS, :] = p
            mixed.append(tap_ref[0, g, layer][None] * p + tap_ref[1, g, layer][None] * prow[layer, g, 1:1 + STEPS, :]
                         + tap_ref[2, g, layer][None] * prow[layer, g, 0:STEPS, :])
        return mixed

    def recent(layer, which, rows_f):
        rrow[layer, which, STEPS - 1:2 * STEPS - 1, :] = rows_f
        total = (lag[layer, which, 0:1] + skip_ref[layer, which][None]) * rows_f
        for back in range(1, STEPS):
            total = total + lag[layer, which, back:back + 1] * rrow[layer, which, STEPS - 1 - back:2 * STEPS - 1 - back, :]
        return total

    def mixer(layer, mixed, hist):
        value = mixed[2].astype(jnp.bfloat16).astype(jnp.float32)
        long_one = hist[:STEPS] + recent(layer, 0, value)
        z_rows = (mixed[0] * long_one).astype(jnp.bfloat16).astype(jnp.float32)
        long_two = hist[STEPS:] + recent(layer, 1, z_rows)
        y_rows = (mixed[1] * long_two).astype(jnp.bfloat16)
        send_sum(2 * layer, jnp.dot(y_rows, wout[layer], preferred_element_type=jnp.float32))
        for g in range(3):
            xb[layer, own, 2 * g:2 * g + 2, :] = prow[layer, g, STEPS:STEPS + 2, :]
        xb[layer, own, 6:8, :] = jnp.zeros((2, chan), jnp.float32)
        xb[layer, own, 8:8 + STEPS, :] = value
        xb[layer, own, 8 + STEPS:8 + 2 * STEPS, :] = z_rows
        for copy in row_copies(layer, own):
            copy.start()

    def mlp(layer, hidden):
        up = jnp.dot(layer_norm(hidden).astype(jnp.bfloat16), wup[layer], preferred_element_type=jnp.float32)
        return jnp.dot(jax.nn.gelu(up).astype(jnp.bfloat16), wdown[layer], preferred_element_type=jnp.float32)

    def put_rows(layer):
        for b in range(SEQ):
            @pl.when(sp != 2 * b + 1)
            def _():
                row_copy(layer, b, 0).wait_recv()

        for b in range(SEQ):
            newrow[2 * STEPS * b:2 * STEPS * (b + 1), 0:chan] = xb[layer, b, 8:16, :]
            for g in range(3):
                st_out[layer, b, g] = xb[layer, b, 2 * g:2 * g + 2, :].astype(jnp.bfloat16)
        turned = jnp.transpose(newrow[...])[:chan]

        @pl.when(sp == 3)
        def _():
            for b in range(SEQ):
                for n, cache in enumerate((v_ref, z_ref)):
                    at = STEPS * (2 * b + n)
                    moved = turned if at == 0 else pltpu.roll(turned, LANES - at, 1)
                    cache[layer, b, :, 0:LANES] = jnp.where(lane_c < STEPS, moved, 0.0).astype(jnp.bfloat16)

    newrow[...] = jnp.zeros_like(newrow)
    rrow[...] = jnp.zeros_like(rrow)
    conv(0, 0, CHUNKS)

    @pl.when(carries)
    def _():
        pl.semaphore_wait(barrier, 6)

    @pl.when(jnp.logical_not(carries))
    def _():
        pl.semaphore_wait(barrier, 3)

    send_hist(0)
    for copy in smalls:
        copy.wait()

    @pl.when(carries)
    def _():
        hidden = jnp.where(own == 0, jnp.concatenate([e_ref[j].astype(jnp.float32)[0:1] for j in range(STEPS)], axis=0),
                           jnp.concatenate([e_ref[j].astype(jnp.float32)[1:2] for j in range(STEPS)], axis=0))
        for layer in range(LAYERS):
            for which in range(2):
                lag[layer, which] = jnp.transpose(lag_ref[layer, which])[:8]
        weight_copy(0, 0).wait()
        mixed = project(0, hidden)
        weight_copy(0, 1).wait()
        mixer(0, mixed, sum_hist(0))
        conv(1, 0, SPLIT)
        weight_copy(0, 2).wait()
        weight_copy(0, 3).wait()
        hidden = hidden + take_sum(0) + bout_ref[0:1]
        send_sum(1, mlp(0, hidden))
        conv(1, SPLIT, CHUNKS)
        send_hist(1)
        weight_copy(1, 0).wait()
        hidden = hidden + take_sum(1)
        mixed = project(1, hidden)
        weight_copy(1, 1).wait()
        mixer(1, mixed, sum_hist(1))
        put_rows(0)
        weight_copy(1, 2).wait()
        weight_copy(1, 3).wait()
        hidden = hidden + take_sum(2) + bout_ref[1:2]
        send_sum(3, mlp(1, hidden))
        put_rows(1)
        fin[own] = hidden + take_sum(3)
        for copy in last_copies(own):
            copy.start()
        for layer in range(LAYERS):
            for copy in row_copies(layer, own):
                copy.wait_send()
        for n in range(4):
            for copy in sum_copies(n):
                copy.wait_send()
        for copy in last_copies(own):
            copy.wait_send()

    @pl.when(jnp.logical_not(carries))
    def _():
        conv(1, 0, CHUNKS)
        send_hist(1)
        for layer in range(LAYERS):
            for n in range(4):
                weight_copy(layer, n).wait()
        put_rows(0)
        put_rows(1)

    for layer in range(LAYERS):
        @pl.when(has_rows)
        def _():
            hist_copy(layer, 1).wait_send()

            @pl.when(sp != 1)
            def _():
                hist_copy(layer, 0).wait_send()

    for b in range(SEQ):
        @pl.when(sp != 2 * b + 1)
        def _():
            last_copy(b, 0).wait_recv()

        for j in range(STEPS):
            hid_out[j, b:b + 1, :] = fin[b, j:j + 1, :]


def emit(hid, v, z, st, hid_o, v_o, z_o, st_o, sem):
    copies = []
    for layer in range(LAYERS):
        for b in range(SEQ):
            copies += [(v.at[layer, b], v_o.at[layer, b]), (z.at[layer, b], z_o.at[layer, b])]
    copies += [(hid, hid_o), (st, st_o)]
    copies = [pltpu.make_async_copy(src, dst, sem.at[n]) for n, (src, dst) in enumerate(copies)]
    for copy in copies:
        copy.start()
    for copy in copies:
        copy.wait()


def solution(mesh):
    def device_fn(step_emb, v_cache, z_cache, short_state, w_in, b_in, short_taps, long_filt, skip_gain, w_out, b_out, w_up, w_down):
        chan = v_cache.shape[3]
        shard_len = v_cache.shape[2]
        model = step_emb.shape[2]
        args = (
            step_emb,
            jnp.swapaxes(v_cache, 2, 3),
            jnp.swapaxes(z_cache, 2, 3),
            jnp.transpose(short_state, (0, 1, 3, 2, 4)),
            jnp.transpose(w_in, (0, 2, 3, 1)),
            jnp.transpose(b_in, (1, 0, 2)),
            jnp.transpose(short_taps, (1, 2, 0, 3)),
            jnp.swapaxes(long_filt, 2, 3),
            skip_gain,
            w_out,
            b_out,
            w_up,
            w_down,
        )
        args = tuple(pltpu.with_memory_space_constraint(arg, pltpu.HBM) for arg in args)
        f32, bf16 = jnp.float32, jnp.bfloat16
        dma = pltpu.SemaphoreType.DMA
        hid, v_out, z_out, st_out = pl.pallas_call(
            kernel,
            out_shape=(
                jax.ShapeDtypeStruct(step_emb.shape, f32),
                pltpu.VMEM(args[1].shape, bf16),
                pltpu.VMEM(args[2].shape, bf16),
                jax.ShapeDtypeStruct(args[3].shape, bf16),
            ),
            in_specs=[pl.BlockSpec(memory_space=pltpu.HBM)] * 13,
            out_specs=[pl.BlockSpec(memory_space=pltpu.VMEM)] * 4,
            scratch_shapes=[
                pltpu.VMEM(step_emb.shape, bf16),
                pltpu.VMEM(args[3].shape, bf16),
                pltpu.VMEM(args[4].shape, bf16),
                pltpu.VMEM(args[5].shape, f32),
                pltpu.VMEM(args[6].shape, f32),
                pltpu.VMEM((LAYERS, 2, chan, shard_len + LANES), f32),
                pltpu.VMEM((LAYERS, 2, chan, LANES), f32),
                pltpu.VMEM(skip_gain.shape, f32),
                pltpu.VMEM(w_out.shape, bf16),
                pltpu.VMEM(b_out.shape, f32),
                pltpu.VMEM(w_up.shape, bf16),
                pltpu.VMEM(w_down.shape, bf16),
                pltpu.VMEM((2, chan, ROWS * LANES), f32),
                pltpu.VMEM((chan, LANES), f32),
                pltpu.VMEM((LAYERS, 2, 8, chan), f32),
                pltpu.VMEM((LAYERS, 3, 8, chan), f32),
                pltpu.VMEM((LAYERS, 2, 8, chan), f32),
                pltpu.VMEM((LANES, 2 * LANES), f32),
                pltpu.VMEM((LAYERS, 4, SEQ, 2 * STEPS, chan), f32),
                pltpu.VMEM((4, 4, STEPS, model), f32),
                pltpu.VMEM((LAYERS, SEQ, 16, chan), f32),
                pltpu.VMEM((SEQ, STEPS, model), f32),
                dma((7,)),
                dma((LAYERS, CHUNKS, 3)),
                dma((LAYERS, 4)),
                dma((LAYERS, SEQ)),
                dma((LAYERS, 4)),
                dma((4, 3)),
                dma((4, 4)),
                dma((LAYERS, 3)),
                dma((LAYERS, SEQ)),
                dma((3,)),
                dma((SEQ,)),
            ],
            compiler_params=pltpu.CompilerParams(collective_id=0, has_side_effects=True, vmem_limit_bytes=40 * 1024 * 1024),
            name="decode",
        )(*args)
        hid, v_out, z_out, st_out = pl.pallas_call(
            emit,
            out_shape=(
                jax.ShapeDtypeStruct(hid.shape, f32),
                jax.ShapeDtypeStruct(v_out.shape, bf16),
                jax.ShapeDtypeStruct(z_out.shape, bf16),
                jax.ShapeDtypeStruct(st_out.shape, bf16),
            ),
            in_specs=[pl.BlockSpec(memory_space=pltpu.VMEM)] * 4,
            out_specs=[pl.BlockSpec(memory_space=pltpu.HBM)] * 4,
            scratch_shapes=[dma((4 * LAYERS + 2,))],
            compiler_params=pltpu.CompilerParams(vmem_limit_bytes=1024 * 1024),
            name="emit",
        )(hid, v_out, z_out, st_out)
        return (hid, jnp.swapaxes(v_out, 2, 3), jnp.swapaxes(z_out, 2, 3), jnp.transpose(st_out, (0, 1, 3, 2, 4)))

    specs_in = (
        P(None, "dp", None),
        P(None, "dp", "sp", "tp"),
        P(None, "dp", "sp", "tp"),
        P(None, "dp", None, None, "tp"),
        P(None, None, None, "tp"),
        P(None, None, "tp"),
        P(None, None, None, "tp"),
        P(None, None, None, "tp"),
        P(None, None, "tp"),
        P(None, "tp", None),
        P(None, None),
        P(None, None, "tp"),
        P(None, "tp", None),
    )
    specs_out = (
        P(None, "dp", None),
        P(None, "dp", "sp", "tp"),
        P(None, "dp", "sp", "tp"),
        P(None, "dp", None, None, "tp"),
    )
    return jax.shard_map(device_fn, mesh=mesh, in_specs=specs_in, out_specs=specs_out, check_vma=False)
```

```python
import functools

import jax
import jax.numpy as jnp
from jax import lax
from jax.experimental import pallas as pl
from jax.experimental.pallas import tpu as pltpu
from jax.sharding import PartitionSpec as P

STEPS = 4
LAYERS = 2
SEQ = 2
ROWS = STEPS * SEQ
LANES = 128
CHUNKS = 12
SPLIT = 4
MESH = pl.DeviceIdType.MESH


def layer_norm(rows_in):
    mean_val = jnp.mean(rows_in, axis=-1, keepdims=True)
    centered = rows_in - mean_val
    var_val = jnp.mean(centered * centered, axis=-1, keepdims=True)
    return centered * lax.rsqrt(var_val + 1e-5)


def kernel(e_hbm, v_hbm, z_hbm, st_hbm, win_hbm, bin_hbm, tap_hbm, h_hbm, skip_hbm, wout_hbm, bout_hbm, wup_hbm, wdown_hbm,
           hid_out, v_ref, z_ref, st_out,
           e_ref, st_ref, win, bin_ref, tap_ref, h_ref, lag_ref, skip_ref, wout, bout_ref, wup, wdown,
           flip, v_even, z_even, v_odd, z_odd, acc, total, lag, prow, rrow, newrow, hx, ar, xb, fin, held,
           small_sem, chunk_sem, w_sem, hsend, hrecv, asend, arecv, xsend, xrecv, fsend, frecv):
    tp = lax.axis_index("tp")
    sp = lax.axis_index("sp")
    own = lax.div(sp, 2)
    carries = lax.rem(sp, 2) == 1
    has_rows = sp != 3
    chan, shard_len = v_hbm.shape[2], v_hbm.shape[3]
    model = e_hbm.shape[2]
    tiles = shard_len // LANES
    rows_per = chan // CHUNKS
    half = lax.div(tp, 2)
    near = tp + 1 - 2 * lax.rem(tp, 2)
    peers = [{"tp": 3 - 3 * half}, {"tp": 2 - half}, {"tp": near}]
    block_peers = [{"sp": lax.rem(sp + d, 4)} for d in (2, 3, 1)]

    barrier = pltpu.get_barrier_semaphore()
    for peer in block_peers:
        pl.semaphore_signal(barrier, inc=1, device_id=peer, device_id_type=MESH)

    @pl.when(carries)
    def _():
        for peer in peers:
            pl.semaphore_signal(barrier, inc=1, device_id=peer, device_id_type=MESH)

    smalls = [pltpu.make_async_copy(src, dst, small_sem.at[n]) for n, (src, dst) in enumerate((
        (e_hbm, e_ref), (st_hbm, st_ref), (bin_hbm, bin_ref), (tap_hbm, tap_ref), (skip_hbm, skip_ref), (bout_hbm, bout_ref),
        (h_hbm.at[:, :, :, pl.ds(0, LANES)], lag_ref)))]
    first = pl.multiple_of(lax.rem(5 - sp, 3) * shard_len, LANES)

    def chunk_copies(layer, k):
        rows = pl.ds(k * rows_per if isinstance(k, int) else pl.multiple_of(k * rows_per, rows_per), rows_per)
        return [
            pltpu.make_async_copy(v_hbm.at[layer, :, rows, :], v_ref.at[layer, :, rows, :], chunk_sem.at[layer, k, 0]),
            pltpu.make_async_copy(z_hbm.at[layer, :, rows, :], z_ref.at[layer, :, rows, :], chunk_sem.at[layer, k, 1]),
            pltpu.make_async_copy(h_hbm.at[layer, :, rows, pl.ds(first, shard_len + LANES)], h_ref.at[layer, :, rows, :],
                                  chunk_sem.at[layer, k, 2]),
        ]

    def weight_copy(layer, n):
        src, dst = ((win_hbm, win), (wout_hbm, wout), (wup_hbm, wup), (wdown_hbm, wdown))[n]
        return pltpu.make_async_copy(src.at[layer], dst.at[layer], w_sem.at[layer, n])

    def start_weights(layer):
        @pl.when(carries)
        def _():
            for n in range(4):
                weight_copy(layer, n).start()

    for n in range(LAYERS * CHUNKS):
        layer, k = divmod(n, CHUNKS)
        for copy in chunk_copies(layer, k):
            copy.start()
        if n == CHUNKS:
            for copy in smalls:
                copy.start()
            start_weights(0)
    start_weights(1)

    lane8 = lax.broadcasted_iota(jnp.int32, (8, LANES), 1)
    lane16 = lax.broadcasted_iota(jnp.int32, (16, LANES), 1)
    spans = range(-1, tiles)

    def turn(cache, layer, row, dst):
        zero = jnp.zeros((16, LANES), jnp.bfloat16)

        def values(b, m):
            return cache[layer, b, pl.ds(row, 16), LANES * m:LANES * (m + 1)] if 0 <= m < tiles else zero

        parts = [jnp.concatenate([values(b, m), values(b, m + 1)], axis=1) for m in spans for b in range(SEQ)]
        dst[...] = jnp.dot(jnp.concatenate(parts, axis=0), flip[...], preferred_element_type=jnp.float32)

    def gather(layer, which, row, src):
        for u in range(2):
            accs = [[None] * SEQ for _ in range(STEPS)]
            after = None
            for m in spans:
                even = h_ref[layer, which, pl.ds(row + 8 * u, 8), LANES * (tiles - 1 - m):LANES * (tiles - m)]
                rolled = pltpu.roll(even, LANES - 1, 1)
                odd = rolled if after is None else jnp.where(lane8 < LANES - 1, rolled, after)
                after = rolled
                for b in range(SEQ):
                    base = 16 * (SEQ * (m + 1) + b) + 8 * u
                    for two in range(2):
                        value = src[base:base + 8, LANES * two:LANES * (two + 1)]
                        for one, taps in enumerate((even, odd)):
                            part = taps * value
                            j = 2 * two + one
                            accs[j][b] = part if accs[j][b] is None else accs[j][b] + part
            for j in range(STEPS):
                for b in range(SEQ):
                    n = SEQ * j + b
                    acc[which, pl.ds(row + 8 * u, 8), LANES * n:LANES * (n + 1)] = accs[j][b]

    def close(row):
        out = jnp.zeros((16, LANES), jnp.float32)
        for which in range(2):
            for j in range(STEPS):
                for b in range(SEQ):
                    n = SEQ * j + b
                    part = jnp.sum(acc[which, pl.ds(row, 16), LANES * n:LANES * (n + 1)], axis=1, keepdims=True)
                    out = jnp.where(lane16 == (2 * b + which) * STEPS + j, part, out)
        total[pl.ds(row, 16), :] = out

    def row_of(k):
        return k * 16 if isinstance(k, int) else pl.multiple_of(k * 16, 16)

    def conv(layer, p0, p1):
        def pair(p, _):
            k = 2 * p
            step = layer * CHUNKS + k + 2
            later, after = lax.rem(lax.div(step, CHUNKS), LAYERS), lax.rem(step, CHUNKS)
            for copy in chunk_copies(layer, k + 1):
                copy.wait()

            @pl.when(step < LAYERS * CHUNKS)
            def _():
                for copy in chunk_copies(later, after):
                    copy.wait()

            @pl.when(has_rows)
            def _():
                r0, r1, r2 = row_of(k), row_of(k + 1), row_of(after)
                turn(v_ref, layer, r1, v_odd)
                gather(layer, 0, r0, v_even)
                turn(z_ref, layer, r1, z_odd)
                gather(layer, 1, r0, z_even)
                turn(v_ref, later, r2, v_even)
                gather(layer, 0, r1, v_odd)
                turn(z_ref, later, r2, z_even)
                gather(layer, 1, r1, z_odd)

            return 0

        lax.fori_loop(p0, p1, pair, 0)

    lane_c = lax.broadcasted_iota(jnp.int32, (chan, LANES), 1)

    def hist_copy(layer, seq):
        return pltpu.make_async_remote_copy(hx.at[layer, sp, seq], hx.at[layer, sp, seq], hsend.at[layer, seq], hrecv.at[layer, sp],
                                            device_id={"sp": 2 * seq + 1}, device_id_type=MESH)

    def send_hist(layer):
        for row in range(0, chan, 16):
            close(row)
        turned = jnp.transpose(total[...])
        for b in range(SEQ):
            hx[layer, sp, b] = turned[2 * STEPS * b:2 * STEPS * (b + 1)]
        hist_copy(layer, 1).start()

        @pl.when(sp != 1)
        def _():
            hist_copy(layer, 0).start()

    def sum_hist(layer):
        for src in range(3):
            @pl.when(sp != src)
            def _():
                pltpu.make_async_remote_copy(hx.at[layer, src, own], hx.at[layer, src, own], hsend.at[layer, 0], hrecv.at[layer, src],
                                             device_id=block_peers[0], device_id_type=MESH).wait_recv()
        return (hx[layer, 0, own] + hx[layer, 1, own]) + hx[layer, 2, own]

    def sum_copies(n):
        return [pltpu.make_async_remote_copy(ar.at[n, tp], ar.at[n, tp], asend.at[n, d], arecv.at[n, tp],
                                             device_id=peers[d], device_id_type=MESH) for d in range(3)]

    def send_sum(n, part):
        ar[n, tp] = part
        for copy in sum_copies(n):
            copy.start()

    def take_sum(n):
        for d in (1, 2, 3):
            src = lax.rem(tp + d, 4)
            pltpu.make_async_remote_copy(ar.at[n, src], ar.at[n, src], asend.at[n, 0], arecv.at[n, src],
                                         device_id=peers[0], device_id_type=MESH).wait_recv()
        return ((ar[n, 0] + ar[n, 1]) + ar[n, 2]) + ar[n, 3]

    def row_copy(layer, seq, d):
        return pltpu.make_async_remote_copy(xb.at[layer, seq], xb.at[layer, seq], xsend.at[layer, d], xrecv.at[layer, seq],
                                            device_id=block_peers[d], device_id_type=MESH)

    def row_copies(layer, seq):
        return [row_copy(layer, seq, d) for d in range(3)]

    def last_copy(seq, d):
        return pltpu.make_async_remote_copy(fin.at[seq], fin.at[seq], fsend.at[d], frecv.at[seq],
                                            device_id=block_peers[d], device_id_type=MESH)

    def last_copies(seq):
        return [last_copy(seq, d) for d in range(3)]

    def project(layer, hidden):
        normed = layer_norm(hidden).astype(jnp.bfloat16)
        mixed = []
        for g in range(3):
            p = lax.dot_general(normed, win[layer, g], (((1,), (1,)), ((), ())), preferred_element_type=jnp.float32)
            p = (p + bin_ref[g, layer][None]).astype(jnp.bfloat16).astype(jnp.float32)
            prow[layer, g, 0:2, :] = st_ref[layer, own, g].astype(jnp.float32)
            prow[layer, g, 2:2 + STEPS, :] = p
            mixed.append(tap_ref[0, g, layer][None] * p + tap_ref[1, g, layer][None] * prow[layer, g, 1:1 + STEPS, :]
                         + tap_ref[2, g, layer][None] * prow[layer, g, 0:STEPS, :])
        return mixed

    def recent(layer, which, rows_f):
        rrow[layer, which, STEPS - 1:2 * STEPS - 1, :] = rows_f
        total = (lag[layer, which, 0:1] + skip_ref[layer, which][None]) * rows_f
        for back in range(1, STEPS):
            total = total + lag[layer, which, back:back + 1] * rrow[layer, which, STEPS - 1 - back:2 * STEPS - 1 - back, :]
        return total

    def mixer(layer, mixed, hist):
        value = mixed[2].astype(jnp.bfloat16).astype(jnp.float32)
        long_one = hist[:STEPS] + recent(layer, 0, value)
        z_rows = (mixed[0] * long_one).astype(jnp.bfloat16).astype(jnp.float32)
        long_two = hist[STEPS:] + recent(layer, 1, z_rows)
        y_rows = (mixed[1] * long_two).astype(jnp.bfloat16)
        send_sum(2 * layer, jnp.dot(y_rows, wout[layer], preferred_element_type=jnp.float32))
        for g in range(3):
            xb[layer, own, 2 * g:2 * g + 2, :] = prow[layer, g, STEPS:STEPS + 2, :]
        xb[layer, own, 6:8, :] = jnp.zeros((2, chan), jnp.float32)
        xb[layer, own, 8:8 + STEPS, :] = value
        xb[layer, own, 8 + STEPS:8 + 2 * STEPS, :] = z_rows
        for copy in row_copies(layer, own):
            copy.start()

    def mlp(layer, hidden):
        up = jnp.dot(layer_norm(hidden).astype(jnp.bfloat16), wup[layer], preferred_element_type=jnp.float32)
        return jnp.dot(jax.nn.gelu(up).astype(jnp.bfloat16), wdown[layer], preferred_element_type=jnp.float32)

    def put_rows(layer):
        for b in range(SEQ):
            @pl.when(sp != 2 * b + 1)
            def _():
                row_copy(layer, b, 0).wait_recv()

        for b in range(SEQ):
            newrow[2 * STEPS * b:2 * STEPS * (b + 1), 0:chan] = xb[layer, b, 8:16, :]
            for g in range(3):
                st_out[layer, b, g] = xb[layer, b, 2 * g:2 * g + 2, :].astype(jnp.bfloat16)
        turned = jnp.transpose(newrow[...])[:chan]

        @pl.when(sp == 3)
        def _():
            for b in range(SEQ):
                for n, cache in enumerate((v_ref, z_ref)):
                    at = STEPS * (2 * b + n)
                    moved = turned if at == 0 else pltpu.roll(turned, LANES - at, 1)
                    cache[layer, b, :, 0:LANES] = jnp.where(lane_c < STEPS, moved, 0.0).astype(jnp.bfloat16)

    newrow[...] = jnp.zeros_like(newrow)
    rrow[...] = jnp.zeros_like(rrow)
    kk = lax.broadcasted_iota(jnp.int32, flip.shape, 0)
    nn = lax.broadcasted_iota(jnp.int32, flip.shape, 1)
    flip[...] = jnp.where(kk == jnp.where(nn < LANES, LANES - nn, 2 * LANES + 2 - nn), 1.0, 0.0).astype(jnp.bfloat16)
    for copy in chunk_copies(0, 0):
        copy.wait()

    @pl.when(has_rows)
    def _():
        turn(v_ref, 0, 0, v_even)
        turn(z_ref, 0, 0, z_even)

    def stage(n, _):
        conv(lax.div(n + 1, 2), SPLIT * lax.div(n, 2), CHUNKS // 2 - (CHUNKS // 2 - SPLIT) * lax.rem(n, 2))

        @pl.when((n == 0) & carries)
        def _():
            pl.semaphore_wait(barrier, 6)

        @pl.when((n == 0) & jnp.logical_not(carries))
        def _():
            pl.semaphore_wait(barrier, 3)

        @pl.when((n != 1) & has_rows)
        def _():
            send_hist(lax.div(n, 2))

        @pl.when(n == 0)
        def _():
            for copy in smalls:
                copy.wait()

        @pl.when((n == 0) & carries)
        def _():
            hidden = jnp.where(own == 0, jnp.concatenate([e_ref[j].astype(jnp.float32)[0:1] for j in range(STEPS)], axis=0),
                               jnp.concatenate([e_ref[j].astype(jnp.float32)[1:2] for j in range(STEPS)], axis=0))
            for layer in range(LAYERS):
                for which in range(2):
                    lag[layer, which] = jnp.transpose(lag_ref[layer, which])[:8]
            weight_copy(0, 0).wait()
            mixed = project(0, hidden)
            weight_copy(0, 1).wait()
            mixer(0, mixed, sum_hist(0))
            held[...] = hidden

        @pl.when((n == 1) & carries)
        def _():
            weight_copy(0, 2).wait()
            weight_copy(0, 3).wait()
            hidden = held[...] + take_sum(0) + bout_ref[0:1]
            send_sum(1, mlp(0, hidden))
            held[...] = hidden

        return 0

    lax.fori_loop(0, 3, stage, 0)

    @pl.when(carries)
    def _():
        weight_copy(1, 0).wait()
        hidden = held[...] + take_sum(1)
        mixed = project(1, hidden)
        weight_copy(1, 1).wait()
        mixer(1, mixed, sum_hist(1))
        put_rows(0)
        weight_copy(1, 2).wait()
        weight_copy(1, 3).wait()
        hidden = hidden + take_sum(2) + bout_ref[1:2]
        send_sum(3, mlp(1, hidden))
        put_rows(1)
        fin[own] = hidden + take_sum(3)
        for copy in last_copies(own):
            copy.start()
        for layer in range(LAYERS):
            for copy in row_copies(layer, own):
                copy.wait_send()
        for n in range(4):
            for copy in sum_copies(n):
                copy.wait_send()
        for copy in last_copies(own):
            copy.wait_send()

    @pl.when(jnp.logical_not(carries))
    def _():
        put_rows(0)
        put_rows(1)

    for layer in range(LAYERS):
        @pl.when(has_rows)
        def _():
            hist_copy(layer, 1).wait_send()

            @pl.when(sp != 1)
            def _():
                hist_copy(layer, 0).wait_send()

    for b in range(SEQ):
        @pl.when(sp != 2 * b + 1)
        def _():
            last_copy(b, 0).wait_recv()

        for j in range(STEPS):
            hid_out[j, b:b + 1, :] = fin[b, j:j + 1, :]


def emit(hid, v, z, st, hid_o, v_o, z_o, st_o, sem):
    copies = []
    for layer in range(LAYERS):
        for b in range(SEQ):
            copies += [(v.at[layer, b], v_o.at[layer, b]), (z.at[layer, b], z_o.at[layer, b])]
    copies += [(hid, hid_o), (st, st_o)]
    copies = [pltpu.make_async_copy(src, dst, sem.at[n]) for n, (src, dst) in enumerate(copies)]
    for copy in copies:
        copy.start()
    for copy in copies:
        copy.wait()


def solution(mesh):
    def device_fn(step_emb, v_cache, z_cache, short_state, w_in, b_in, short_taps, long_filt, skip_gain, w_out, b_out, w_up, w_down):
        chan = v_cache.shape[3]
        shard_len = v_cache.shape[2]
        model = step_emb.shape[2]
        args = (
            step_emb,
            jnp.swapaxes(v_cache, 2, 3),
            jnp.swapaxes(z_cache, 2, 3),
            jnp.transpose(short_state, (0, 1, 3, 2, 4)),
            jnp.transpose(w_in, (0, 2, 3, 1)),
            jnp.transpose(b_in, (1, 0, 2)),
            jnp.transpose(short_taps, (1, 2, 0, 3)),
            jnp.swapaxes(long_filt, 2, 3),
            skip_gain,
            w_out,
            b_out,
            w_up,
            w_down,
        )
        args = tuple(pltpu.with_memory_space_constraint(arg, pltpu.HBM) for arg in args)
        f32, bf16 = jnp.float32, jnp.bfloat16
        dma = pltpu.SemaphoreType.DMA
        hid, v_out, z_out, st_out = pl.pallas_call(
            kernel,
            out_shape=(
                jax.ShapeDtypeStruct(step_emb.shape, f32),
                pltpu.VMEM(args[1].shape, bf16),
                pltpu.VMEM(args[2].shape, bf16),
                jax.ShapeDtypeStruct(args[3].shape, bf16),
            ),
            in_specs=[pl.BlockSpec(memory_space=pltpu.HBM)] * 13,
            out_specs=[pl.BlockSpec(memory_space=pltpu.VMEM)] * 4,
            scratch_shapes=[
                pltpu.VMEM(step_emb.shape, bf16),
                pltpu.VMEM(args[3].shape, bf16),
                pltpu.VMEM(args[4].shape, bf16),
                pltpu.VMEM(args[5].shape, f32),
                pltpu.VMEM(args[6].shape, f32),
                pltpu.VMEM((LAYERS, 2, chan, shard_len + LANES), f32),
                pltpu.VMEM((LAYERS, 2, chan, LANES), f32),
                pltpu.VMEM(skip_gain.shape, f32),
                pltpu.VMEM(w_out.shape, bf16),
                pltpu.VMEM(b_out.shape, f32),
                pltpu.VMEM(w_up.shape, bf16),
                pltpu.VMEM(w_down.shape, bf16),
                pltpu.VMEM((2 * LANES, 2 * LANES), bf16),
                *[pltpu.VMEM((16 * SEQ * (shard_len // LANES + 1), 2 * LANES), f32)] * 4,
                pltpu.VMEM((2, chan, ROWS * LANES), f32),
                pltpu.VMEM((chan, LANES), f32),
                pltpu.VMEM((LAYERS, 2, 8, chan), f32),
                pltpu.VMEM((LAYERS, 3, 8, chan), f32),
                pltpu.VMEM((LAYERS, 2, 8, chan), f32),
                pltpu.VMEM((LANES, 2 * LANES), f32),
                pltpu.VMEM((LAYERS, 4, SEQ, 2 * STEPS, chan), f32),
                pltpu.VMEM((4, 4, STEPS, model), f32),
                pltpu.VMEM((LAYERS, SEQ, 16, chan), f32),
                pltpu.VMEM((SEQ, STEPS, model), f32),
                pltpu.VMEM((STEPS, model), f32),
                dma((7,)),
                dma((LAYERS, CHUNKS, 3)),
                dma((LAYERS, 4)),
                dma((LAYERS, SEQ)),
                dma((LAYERS, 4)),
                dma((4, 3)),
                dma((4, 4)),
                dma((LAYERS, 3)),
                dma((LAYERS, SEQ)),
                dma((3,)),
                dma((SEQ,)),
            ],
            compiler_params=pltpu.CompilerParams(collective_id=0, has_side_effects=True, vmem_limit_bytes=40 * 1024 * 1024),
            name="decode",
        )(*args)
        hid, v_out, z_out, st_out = pl.pallas_call(
            emit,
            out_shape=(
                jax.ShapeDtypeStruct(hid.shape, f32),
                jax.ShapeDtypeStruct(v_out.shape, bf16),
                jax.ShapeDtypeStruct(z_out.shape, bf16),
                jax.ShapeDtypeStruct(st_out.shape, bf16),
            ),
            in_specs=[pl.BlockSpec(memory_space=pltpu.VMEM)] * 4,
            out_specs=[pl.BlockSpec(memory_space=pltpu.HBM)] * 4,
            scratch_shapes=[dma((4 * LAYERS + 2,))],
            compiler_params=pltpu.CompilerParams(vmem_limit_bytes=1024 * 1024),
            name="emit",
        )(hid, v_out, z_out, st_out)
        return (hid, jnp.swapaxes(v_out, 2, 3), jnp.swapaxes(z_out, 2, 3), jnp.transpose(st_out, (0, 1, 3, 2, 4)))

    specs_in = (
        P(None, "dp", None),
        P(None, "dp", "sp", "tp"),
        P(None, "dp", "sp", "tp"),
        P(None, "dp", None, None, "tp"),
        P(None, None, None, "tp"),
        P(None, None, "tp"),
        P(None, None, None, "tp"),
        P(None, None, None, "tp"),
        P(None, None, "tp"),
        P(None, "tp", None),
        P(None, None),
        P(None, None, "tp"),
        P(None, "tp", None),
    )
    specs_out = (
        P(None, "dp", None),
        P(None, "dp", "sp", "tp"),
        P(None, "dp", "sp", "tp"),
        P(None, "dp", None, None, "tp"),
    )
    return jax.shard_map(device_fn, mesh=mesh, in_specs=specs_in, out_specs=specs_out, check_vma=False)
```

```python
import functools

import jax
import jax.numpy as jnp
from jax import lax
from jax.experimental import pallas as pl
from jax.experimental.pallas import tpu as pltpu
from jax.sharding import PartitionSpec as P

STEPS = 4
LAYERS = 2
SEQ = 2
ROWS = STEPS * SEQ
LANES = 128
CHUNKS = 12
FIRST, SECOND = 2, 3
MESH = pl.DeviceIdType.MESH


def layer_norm(rows_in):
    mean_val = jnp.mean(rows_in, axis=-1, keepdims=True)
    centered = rows_in - mean_val
    var_val = jnp.mean(centered * centered, axis=-1, keepdims=True)
    return centered * lax.rsqrt(var_val + 1e-5)


def kernel(e_hbm, v_hbm, z_hbm, st_hbm, win_hbm, bin_hbm, tap_hbm, h_hbm, skip_hbm, wout_hbm, bout_hbm, wup_hbm, wdown_hbm,
           hid_out, v_ref, z_ref, st_out,
           e_ref, st_ref, win, bin_ref, tap_ref, h_ref, lag_ref, skip_ref, wout, bout_ref, wup, wdown,
           flip, v_even, z_even, v_odd, z_odd, acc, total, lag, prow, rrow, newrow, hx, ar, xb, fin, held, mixed_ref,
           small_sem, chunk_sem, w_sem, hsend, hrecv, asend, arecv, xsend, xrecv, fsend, frecv):
    tp = lax.axis_index("tp")
    sp = lax.axis_index("sp")
    own = lax.div(sp, 2)
    carries = lax.rem(sp, 2) == 1
    has_rows = sp != 3
    chan, shard_len = v_hbm.shape[2], v_hbm.shape[3]
    model = e_hbm.shape[2]
    tiles = shard_len // LANES
    rows_per = chan // CHUNKS
    half = lax.div(tp, 2)
    near = tp + 1 - 2 * lax.rem(tp, 2)
    peers = [{"tp": 3 - 3 * half}, {"tp": 2 - half}, {"tp": near}]
    block_peers = [{"sp": lax.rem(sp + d, 4)} for d in (2, 3, 1)]

    barrier = pltpu.get_barrier_semaphore()
    for peer in block_peers:
        pl.semaphore_signal(barrier, inc=1, device_id=peer, device_id_type=MESH)

    @pl.when(carries)
    def _():
        for peer in peers:
            pl.semaphore_signal(barrier, inc=1, device_id=peer, device_id_type=MESH)

    smalls = [pltpu.make_async_copy(src, dst, small_sem.at[n]) for n, (src, dst) in enumerate((
        (e_hbm, e_ref), (st_hbm, st_ref), (bin_hbm, bin_ref), (tap_hbm, tap_ref), (skip_hbm, skip_ref), (bout_hbm, bout_ref),
        (h_hbm.at[:, :, :, pl.ds(0, LANES)], lag_ref)))]
    first = pl.multiple_of(lax.rem(5 - sp, 3) * shard_len, LANES)

    def chunk_copies(layer, k):
        rows = pl.ds(k * rows_per if isinstance(k, int) else pl.multiple_of(k * rows_per, rows_per), rows_per)
        return [
            pltpu.make_async_copy(v_hbm.at[layer, :, rows, :], v_ref.at[layer, :, rows, :], chunk_sem.at[layer, k, 0]),
            pltpu.make_async_copy(z_hbm.at[layer, :, rows, :], z_ref.at[layer, :, rows, :], chunk_sem.at[layer, k, 1]),
            pltpu.make_async_copy(h_hbm.at[layer, :, rows, pl.ds(first, shard_len + LANES)], h_ref.at[layer, :, rows, :],
                                  chunk_sem.at[layer, k, 2]),
        ]

    def weight_copy(layer, n):
        src, dst = ((win_hbm, win), (wout_hbm, wout), (wup_hbm, wup), (wdown_hbm, wdown))[n]
        return pltpu.make_async_copy(src.at[layer], dst.at[layer], w_sem.at[layer, n])

    def start_weights(layer):
        @pl.when(carries)
        def _():
            for n in range(4):
                weight_copy(layer, n).start()

    for n in range(LAYERS * CHUNKS):
        layer, k = divmod(n, CHUNKS)
        for copy in chunk_copies(layer, k):
            copy.start()
        if n == CHUNKS:
            for copy in smalls:
                copy.start()
            start_weights(0)
    start_weights(1)

    lane8 = lax.broadcasted_iota(jnp.int32, (8, LANES), 1)
    lane16 = lax.broadcasted_iota(jnp.int32, (16, LANES), 1)
    spans = range(-1, tiles)

    def turn(cache, layer, row, dst):
        zero = jnp.zeros((16, LANES), jnp.bfloat16)

        def values(b, m):
            return cache[layer, b, pl.ds(row, 16), LANES * m:LANES * (m + 1)] if 0 <= m < tiles else zero

        parts = [jnp.concatenate([values(b, m), values(b, m + 1)], axis=1) for m in spans for b in range(SEQ)]
        dst[...] = jnp.dot(jnp.concatenate(parts, axis=0), flip[...], preferred_element_type=jnp.float32)

    def gather(layer, which, row, src):
        for u in range(2):
            accs = [[None] * SEQ for _ in range(STEPS)]
            after = None
            for m in spans:
                even = h_ref[layer, which, pl.ds(row + 8 * u, 8), LANES * (tiles - 1 - m):LANES * (tiles - m)]
                rolled = pltpu.roll(even, LANES - 1, 1)
                odd = rolled if after is None else jnp.where(lane8 < LANES - 1, rolled, after)
                after = rolled
                for b in range(SEQ):
                    base = 16 * (SEQ * (m + 1) + b) + 8 * u
                    for two in range(2):
                        value = src[base:base + 8, LANES * two:LANES * (two + 1)]
                        for one, taps in enumerate((even, odd)):
                            part = taps * value
                            j = 2 * two + one
                            accs[j][b] = part if accs[j][b] is None else accs[j][b] + part
            for j in range(STEPS):
                for b in range(SEQ):
                    n = SEQ * j + b
                    acc[which, pl.ds(row + 8 * u, 8), LANES * n:LANES * (n + 1)] = accs[j][b]

    def close(row):
        out = jnp.zeros((16, LANES), jnp.float32)
        for which in range(2):
            for j in range(STEPS):
                for b in range(SEQ):
                    n = SEQ * j + b
                    part = jnp.sum(acc[which, pl.ds(row, 16), LANES * n:LANES * (n + 1)], axis=1, keepdims=True)
                    out = jnp.where(lane16 == (2 * b + which) * STEPS + j, part, out)
        total[pl.ds(row, 16), :] = out

    def row_of(k):
        return k * 16 if isinstance(k, int) else pl.multiple_of(k * 16, 16)

    def conv(layer, p0, p1):
        def pair(p, _):
            k = 2 * p
            step = layer * CHUNKS + k + 2
            later, after = lax.rem(lax.div(step, CHUNKS), LAYERS), lax.rem(step, CHUNKS)
            for copy in chunk_copies(layer, k + 1):
                copy.wait()

            @pl.when(step < LAYERS * CHUNKS)
            def _():
                for copy in chunk_copies(later, after):
                    copy.wait()

            @pl.when(has_rows)
            def _():
                r0, r1, r2 = row_of(k), row_of(k + 1), row_of(after)
                turn(v_ref, layer, r1, v_odd)
                gather(layer, 0, r0, v_even)
                turn(z_ref, layer, r1, z_odd)
                gather(layer, 1, r0, z_even)
                turn(v_ref, later, r2, v_even)
                gather(layer, 0, r1, v_odd)
                turn(z_ref, later, r2, z_even)
                gather(layer, 1, r1, z_odd)

            return 0

        lax.fori_loop(p0, p1, pair, 0)

    lane_c = lax.broadcasted_iota(jnp.int32, (chan, LANES), 1)

    def hist_copy(layer, seq):
        return pltpu.make_async_remote_copy(hx.at[layer, sp, seq], hx.at[layer, sp, seq], hsend.at[layer, seq], hrecv.at[layer, sp],
                                            device_id={"sp": 2 * seq + 1}, device_id_type=MESH)

    def send_hist(layer):
        for row in range(0, chan, 16):
            close(row)
        turned = jnp.transpose(total[...])
        for b in range(SEQ):
            hx[layer, sp, b] = turned[2 * STEPS * b:2 * STEPS * (b + 1)]
        hist_copy(layer, 1).start()

        @pl.when(sp != 1)
        def _():
            hist_copy(layer, 0).start()

    def sum_hist(layer):
        for src in range(3):
            @pl.when(sp != src)
            def _():
                pltpu.make_async_remote_copy(hx.at[layer, src, own], hx.at[layer, src, own], hsend.at[layer, 0], hrecv.at[layer, src],
                                             device_id=block_peers[0], device_id_type=MESH).wait_recv()
        return (hx[layer, 0, own] + hx[layer, 1, own]) + hx[layer, 2, own]

    def sum_copies(n):
        return [pltpu.make_async_remote_copy(ar.at[n, tp], ar.at[n, tp], asend.at[n, d], arecv.at[n, tp],
                                             device_id=peers[d], device_id_type=MESH) for d in range(3)]

    def send_sum(n, part):
        ar[n, tp] = part
        for copy in sum_copies(n):
            copy.start()

    def take_sum(n):
        for d in (1, 2, 3):
            src = lax.rem(tp + d, 4)
            pltpu.make_async_remote_copy(ar.at[n, src], ar.at[n, src], asend.at[n, 0], arecv.at[n, src],
                                         device_id=peers[0], device_id_type=MESH).wait_recv()
        return ((ar[n, 0] + ar[n, 1]) + ar[n, 2]) + ar[n, 3]

    def row_copy(layer, seq, d):
        return pltpu.make_async_remote_copy(xb.at[layer, seq], xb.at[layer, seq], xsend.at[layer, d], xrecv.at[layer, seq],
                                            device_id=block_peers[d], device_id_type=MESH)

    def row_copies(layer, seq):
        return [row_copy(layer, seq, d) for d in range(3)]

    def last_copy(seq, d):
        return pltpu.make_async_remote_copy(fin.at[seq], fin.at[seq], fsend.at[d], frecv.at[seq],
                                            device_id=block_peers[d], device_id_type=MESH)

    def last_copies(seq):
        return [last_copy(seq, d) for d in range(3)]

    def project(layer, hidden):
        normed = layer_norm(hidden).astype(jnp.bfloat16)
        mixed = []
        for g in range(3):
            p = lax.dot_general(normed, win[layer, g], (((1,), (1,)), ((), ())), preferred_element_type=jnp.float32)
            p = (p + bin_ref[g, layer][None]).astype(jnp.bfloat16).astype(jnp.float32)
            prow[layer, g, 0:2, :] = st_ref[layer, own, g].astype(jnp.float32)
            prow[layer, g, 2:2 + STEPS, :] = p
            mixed.append(tap_ref[0, g, layer][None] * p + tap_ref[1, g, layer][None] * prow[layer, g, 1:1 + STEPS, :]
                         + tap_ref[2, g, layer][None] * prow[layer, g, 0:STEPS, :])
        return mixed

    def recent(layer, which, rows_f):
        rrow[layer, which, STEPS - 1:2 * STEPS - 1, :] = rows_f
        total = (lag[layer, which, 0:1] + skip_ref[layer, which][None]) * rows_f
        for back in range(1, STEPS):
            total = total + lag[layer, which, back:back + 1] * rrow[layer, which, STEPS - 1 - back:2 * STEPS - 1 - back, :]
        return total

    def mixer(layer, mixed, hist):
        value = mixed[2].astype(jnp.bfloat16).astype(jnp.float32)
        long_one = hist[:STEPS] + recent(layer, 0, value)
        z_rows = (mixed[0] * long_one).astype(jnp.bfloat16).astype(jnp.float32)
        long_two = hist[STEPS:] + recent(layer, 1, z_rows)
        y_rows = (mixed[1] * long_two).astype(jnp.bfloat16)
        send_sum(2 * layer, jnp.dot(y_rows, wout[layer], preferred_element_type=jnp.float32))
        for g in range(3):
            xb[layer, own, 2 * g:2 * g + 2, :] = prow[layer, g, STEPS:STEPS + 2, :]
        xb[layer, own, 6:8, :] = jnp.zeros((2, chan), jnp.float32)
        xb[layer, own, 8:8 + STEPS, :] = value
        xb[layer, own, 8 + STEPS:8 + 2 * STEPS, :] = z_rows
        for copy in row_copies(layer, own):
            copy.start()

    def mlp(layer, hidden):
        up = jnp.dot(layer_norm(hidden).astype(jnp.bfloat16), wup[layer], preferred_element_type=jnp.float32)
        return jnp.dot(jax.nn.gelu(up).astype(jnp.bfloat16), wdown[layer], preferred_element_type=jnp.float32)

    def put_rows(layer):
        for b in range(SEQ):
            @pl.when(sp != 2 * b + 1)
            def _():
                row_copy(layer, b, 0).wait_recv()

        for b in range(SEQ):
            newrow[2 * STEPS * b:2 * STEPS * (b + 1), 0:chan] = xb[layer, b, 8:16, :]
            for g in range(3):
                st_out[layer, b, g] = xb[layer, b, 2 * g:2 * g + 2, :].astype(jnp.bfloat16)
        turned = jnp.transpose(newrow[...])[:chan]

        @pl.when(sp == 3)
        def _():
            for b in range(SEQ):
                for n, cache in enumerate((v_ref, z_ref)):
                    at = STEPS * (2 * b + n)
                    moved = turned if at == 0 else pltpu.roll(turned, LANES - at, 1)
                    cache[layer, b, :, 0:LANES] = jnp.where(lane_c < STEPS, moved, 0.0).astype(jnp.bfloat16)

    newrow[...] = jnp.zeros_like(newrow)
    rrow[...] = jnp.zeros_like(rrow)
    kk = lax.broadcasted_iota(jnp.int32, flip.shape, 0)
    nn = lax.broadcasted_iota(jnp.int32, flip.shape, 1)
    flip[...] = jnp.where(kk == jnp.where(nn < LANES, LANES - nn, 2 * LANES + 2 - nn), 1.0, 0.0).astype(jnp.bfloat16)
    for copy in chunk_copies(0, 0):
        copy.wait()

    @pl.when(has_rows)
    def _():
        turn(v_ref, 0, 0, v_even)
        turn(z_ref, 0, 0, z_even)

    def stage(n, _):
        at_least = [None] + [lax.div(n + 3 - i, 3) if i == 1 else lax.div(n, i) for i in (1, 2, 3)]
        conv(at_least[1], FIRST * at_least[2] + SECOND * at_least[3],
             CHUNKS // 2 - (CHUNKS // 2 - FIRST) * (at_least[1] - at_least[2])
             - (CHUNKS // 2 - FIRST - SECOND) * (at_least[2] - at_least[3]))

        @pl.when((n == 0) & carries)
        def _():
            pl.semaphore_wait(barrier, 6)

        @pl.when((n == 0) & jnp.logical_not(carries))
        def _():
            pl.semaphore_wait(barrier, 3)

        @pl.when(((n == 0) | (n == 3)) & has_rows)
        def _():
            send_hist(lax.div(n, 3))

        @pl.when(n == 0)
        def _():
            for copy in smalls:
                copy.wait()

        @pl.when((n == 0) & carries)
        def _():
            hidden = jnp.where(own == 0, jnp.concatenate([e_ref[j].astype(jnp.float32)[0:1] for j in range(STEPS)], axis=0),
                               jnp.concatenate([e_ref[j].astype(jnp.float32)[1:2] for j in range(STEPS)], axis=0))
            held[...] = hidden
            weight_copy(0, 0).wait()
            for g, rows_f in enumerate(project(0, hidden)):
                mixed_ref[g] = rows_f
            for layer in range(LAYERS):
                for which in range(2):
                    lag[layer, which] = jnp.transpose(lag_ref[layer, which])[:8]
            for n_w in (1, 2, 3):
                weight_copy(0, n_w).wait()

        @pl.when((n == 1) & carries)
        def _():
            mixer(0, [mixed_ref[g] for g in range(3)], sum_hist(0))

        @pl.when((n == 2) & carries)
        def _():
            hidden = held[...] + take_sum(0) + bout_ref[0:1]
            send_sum(1, mlp(0, hidden))
            held[...] = hidden

        return 0

    lax.fori_loop(0, 4, stage, 0)

    @pl.when(carries)
    def _():
        weight_copy(1, 0).wait()
        hidden = held[...] + take_sum(1)
        mixed = project(1, hidden)
        weight_copy(1, 1).wait()
        mixer(1, mixed, sum_hist(1))
        put_rows(0)
        weight_copy(1, 2).wait()
        weight_copy(1, 3).wait()
        hidden = hidden + take_sum(2) + bout_ref[1:2]
        send_sum(3, mlp(1, hidden))
        put_rows(1)
        fin[own] = hidden + take_sum(3)
        for copy in last_copies(own):
            copy.start()
        for layer in range(LAYERS):
            for copy in row_copies(layer, own):
                copy.wait_send()
        for n in range(4):
            for copy in sum_copies(n):
                copy.wait_send()
        for copy in last_copies(own):
            copy.wait_send()

    @pl.when(jnp.logical_not(carries))
    def _():
        put_rows(0)
        put_rows(1)

    for layer in range(LAYERS):
        @pl.when(has_rows)
        def _():
            hist_copy(layer, 1).wait_send()

            @pl.when(sp != 1)
            def _():
                hist_copy(layer, 0).wait_send()

    for b in range(SEQ):
        @pl.when(sp != 2 * b + 1)
        def _():
            last_copy(b, 0).wait_recv()

        for j in range(STEPS):
            hid_out[j, b:b + 1, :] = fin[b, j:j + 1, :]


def emit(hid, v, z, st, hid_o, v_o, z_o, st_o, sem):
    copies = []
    for layer in range(LAYERS):
        for b in range(SEQ):
            copies += [(v.at[layer, b], v_o.at[layer, b]), (z.at[layer, b], z_o.at[layer, b])]
    copies += [(hid, hid_o), (st, st_o)]
    copies = [pltpu.make_async_copy(src, dst, sem.at[n]) for n, (src, dst) in enumerate(copies)]
    for copy in copies:
        copy.start()
    for copy in copies:
        copy.wait()


def solution(mesh):
    def device_fn(step_emb, v_cache, z_cache, short_state, w_in, b_in, short_taps, long_filt, skip_gain, w_out, b_out, w_up, w_down):
        chan = v_cache.shape[3]
        shard_len = v_cache.shape[2]
        model = step_emb.shape[2]
        args = (
            step_emb,
            jnp.swapaxes(v_cache, 2, 3),
            jnp.swapaxes(z_cache, 2, 3),
            jnp.transpose(short_state, (0, 1, 3, 2, 4)),
            jnp.transpose(w_in, (0, 2, 3, 1)),
            jnp.transpose(b_in, (1, 0, 2)),
            jnp.transpose(short_taps, (1, 2, 0, 3)),
            jnp.swapaxes(long_filt, 2, 3),
            skip_gain,
            w_out,
            b_out,
            w_up,
            w_down,
        )
        args = tuple(pltpu.with_memory_space_constraint(arg, pltpu.HBM) for arg in args)
        f32, bf16 = jnp.float32, jnp.bfloat16
        dma = pltpu.SemaphoreType.DMA
        hid, v_out, z_out, st_out = pl.pallas_call(
            kernel,
            out_shape=(
                jax.ShapeDtypeStruct(step_emb.shape, f32),
                pltpu.VMEM(args[1].shape, bf16),
                pltpu.VMEM(args[2].shape, bf16),
                jax.ShapeDtypeStruct(args[3].shape, bf16),
            ),
            in_specs=[pl.BlockSpec(memory_space=pltpu.HBM)] * 13,
            out_specs=[pl.BlockSpec(memory_space=pltpu.VMEM)] * 4,
            scratch_shapes=[
                pltpu.VMEM(step_emb.shape, bf16),
                pltpu.VMEM(args[3].shape, bf16),
                pltpu.VMEM(args[4].shape, bf16),
                pltpu.VMEM(args[5].shape, f32),
                pltpu.VMEM(args[6].shape, f32),
                pltpu.VMEM((LAYERS, 2, chan, shard_len + LANES), f32),
                pltpu.VMEM((LAYERS, 2, chan, LANES), f32),
                pltpu.VMEM(skip_gain.shape, f32),
                pltpu.VMEM(w_out.shape, bf16),
                pltpu.VMEM(b_out.shape, f32),
                pltpu.VMEM(w_up.shape, bf16),
                pltpu.VMEM(w_down.shape, bf16),
                pltpu.VMEM((2 * LANES, 2 * LANES), bf16),
                *[pltpu.VMEM((16 * SEQ * (shard_len // LANES + 1), 2 * LANES), f32)] * 4,
                pltpu.VMEM((2, chan, ROWS * LANES), f32),
                pltpu.VMEM((chan, LANES), f32),
                pltpu.VMEM((LAYERS, 2, 8, chan), f32),
                pltpu.VMEM((LAYERS, 3, 8, chan), f32),
                pltpu.VMEM((LAYERS, 2, 8, chan), f32),
                pltpu.VMEM((LANES, 2 * LANES), f32),
                pltpu.VMEM((LAYERS, 4, SEQ, 2 * STEPS, chan), f32),
                pltpu.VMEM((4, 4, STEPS, model), f32),
                pltpu.VMEM((LAYERS, SEQ, 16, chan), f32),
                pltpu.VMEM((SEQ, STEPS, model), f32),
                pltpu.VMEM((STEPS, model), f32),
                pltpu.VMEM((3, STEPS, chan), f32),
                dma((7,)),
                dma((LAYERS, CHUNKS, 3)),
                dma((LAYERS, 4)),
                dma((LAYERS, SEQ)),
                dma((LAYERS, 4)),
                dma((4, 3)),
                dma((4, 4)),
                dma((LAYERS, 3)),
                dma((LAYERS, SEQ)),
                dma((3,)),
                dma((SEQ,)),
            ],
            compiler_params=pltpu.CompilerParams(collective_id=0, has_side_effects=True, vmem_limit_bytes=40 * 1024 * 1024),
            name="decode",
        )(*args)
        hid, v_out, z_out, st_out = pl.pallas_call(
            emit,
            out_shape=(
                jax.ShapeDtypeStruct(hid.shape, f32),
                jax.ShapeDtypeStruct(v_out.shape, bf16),
                jax.ShapeDtypeStruct(z_out.shape, bf16),
                jax.ShapeDtypeStruct(st_out.shape, bf16),
            ),
            in_specs=[pl.BlockSpec(memory_space=pltpu.VMEM)] * 4,
            out_specs=[pl.BlockSpec(memory_space=pltpu.HBM)] * 4,
            scratch_shapes=[dma((4 * LAYERS + 2,))],
            compiler_params=pltpu.CompilerParams(vmem_limit_bytes=1024 * 1024),
            name="emit",
        )(hid, v_out, z_out, st_out)
        return (hid, jnp.swapaxes(v_out, 2, 3), jnp.swapaxes(z_out, 2, 3), jnp.transpose(st_out, (0, 1, 3, 2, 4)))

    specs_in = (
        P(None, "dp", None),
        P(None, "dp", "sp", "tp"),
        P(None, "dp", "sp", "tp"),
        P(None, "dp", None, None, "tp"),
        P(None, None, None, "tp"),
        P(None, None, "tp"),
        P(None, None, None, "tp"),
        P(None, None, None, "tp"),
        P(None, None, "tp"),
        P(None, "tp", None),
        P(None, None),
        P(None, None, "tp"),
        P(None, "tp", None),
    )
    specs_out = (
        P(None, "dp", None),
        P(None, "dp", "sp", "tp"),
        P(None, "dp", "sp", "tp"),
        P(None, "dp", None, None, "tp"),
    )
    return jax.shard_map(device_fn, mesh=mesh, in_specs=specs_in, out_specs=specs_out, check_vma=False)
```

```python
import functools

import jax
import jax.numpy as jnp
from jax import lax
from jax.experimental import pallas as pl
from jax.experimental.pallas import tpu as pltpu
from jax.sharding import PartitionSpec as P

STEPS = 4
LAYERS = 2
SEQ = 2
ROWS = STEPS * SEQ
LANES = 128
CHUNKS = 12
FIRST, SECOND = 2, 3
AHEAD = 6
MESH = pl.DeviceIdType.MESH


def layer_norm(rows_in):
    mean_val = jnp.mean(rows_in, axis=-1, keepdims=True)
    centered = rows_in - mean_val
    var_val = jnp.mean(centered * centered, axis=-1, keepdims=True)
    return centered * lax.rsqrt(var_val + 1e-5)


def kernel(e_hbm, v_hbm, z_hbm, st_hbm, win_hbm, bin_hbm, tap_hbm, h_hbm, skip_hbm, wout_hbm, bout_hbm, wup_hbm, wdown_hbm,
           hid_out, v_ref, z_ref, st_out,
           e_ref, st_ref, win, bin_ref, tap_ref, h_ref, lag_ref, skip_ref, wout, bout_ref, wup, wdown,
           flip, v_even, z_even, v_odd, z_odd, acc, total, lag, prow, rrow, newrow, hx, ar, xb, fin, held, mixed_ref,
           small_sem, chunk_sem, w_sem, hsend, hrecv, asend, arecv, xsend, xrecv, fsend, frecv):
    tp = lax.axis_index("tp")
    sp = lax.axis_index("sp")
    own = lax.div(sp, 2)
    carries = lax.rem(sp, 2) == 1
    has_rows = sp != 3
    chan, shard_len = v_hbm.shape[2], v_hbm.shape[3]
    model = e_hbm.shape[2]
    tiles = shard_len // LANES
    rows_per = chan // CHUNKS
    half = lax.div(tp, 2)
    near = tp + 1 - 2 * lax.rem(tp, 2)
    peers = [{"tp": 3 - 3 * half}, {"tp": 2 - half}, {"tp": near}]
    block_peers = [{"sp": lax.rem(sp + d, 4)} for d in (2, 3, 1)]

    barrier = pltpu.get_barrier_semaphore()
    for peer in block_peers:
        pl.semaphore_signal(barrier, inc=1, device_id=peer, device_id_type=MESH)

    @pl.when(carries)
    def _():
        for peer in peers:
            pl.semaphore_signal(barrier, inc=1, device_id=peer, device_id_type=MESH)

    smalls = [pltpu.make_async_copy(src, dst, small_sem.at[n]) for n, (src, dst) in enumerate((
        (e_hbm, e_ref), (st_hbm, st_ref), (bin_hbm, bin_ref), (tap_hbm, tap_ref), (skip_hbm, skip_ref), (bout_hbm, bout_ref),
        (h_hbm.at[:, :, :, pl.ds(0, LANES)], lag_ref)))]
    first = pl.multiple_of(lax.rem(5 - sp, 3) * shard_len, LANES)

    def chunk_copies(layer, k):
        rows = pl.ds(k * rows_per if isinstance(k, int) else pl.multiple_of(k * rows_per, rows_per), rows_per)
        return [
            pltpu.make_async_copy(v_hbm.at[layer, :, rows, :], v_ref.at[layer, :, rows, :], chunk_sem.at[layer, k, 0]),
            pltpu.make_async_copy(z_hbm.at[layer, :, rows, :], z_ref.at[layer, :, rows, :], chunk_sem.at[layer, k, 1]),
            pltpu.make_async_copy(h_hbm.at[layer, :, rows, pl.ds(first, shard_len + LANES)], h_ref.at[layer, :, rows, :],
                                  chunk_sem.at[layer, k, 2]),
        ]

    def weight_copy(layer, n):
        src, dst = ((win_hbm, win), (wout_hbm, wout), (wup_hbm, wup), (wdown_hbm, wdown))[n]
        return pltpu.make_async_copy(src.at[layer], dst.at[layer], w_sem.at[layer, n])

    def start_weights(layer):
        @pl.when(carries)
        def _():
            for n in range(4):
                weight_copy(layer, n).start()

    for k in range(AHEAD):
        for copy in chunk_copies(0, k):
            copy.start()

    def start_ahead(layer, p):
        for n in range(2):
            step = layer * CHUNKS + 2 * p + AHEAD + n

            @pl.when(step < LAYERS * CHUNKS)
            def _():
                for copy in chunk_copies(lax.div(step, CHUNKS), lax.rem(step, CHUNKS)):
                    copy.start()

        @pl.when((layer == 0) & (p == 1))
        def _():
            for copy in smalls:
                copy.start()

        @pl.when((layer == 0) & (p == 2))
        def _():
            start_weights(0)

        @pl.when((layer == 1) & (p == 1))
        def _():
            start_weights(1)

    lane8 = lax.broadcasted_iota(jnp.int32, (8, LANES), 1)
    lane16 = lax.broadcasted_iota(jnp.int32, (16, LANES), 1)
    spans = range(-1, tiles)

    def turn(cache, layer, row, dst):
        zero = jnp.zeros((16, LANES), jnp.bfloat16)

        def values(b, m):
            return cache[layer, b, pl.ds(row, 16), LANES * m:LANES * (m + 1)] if 0 <= m < tiles else zero

        parts = [jnp.concatenate([values(b, m), values(b, m + 1)], axis=1) for m in spans for b in range(SEQ)]
        dst[...] = jnp.dot(jnp.concatenate(parts, axis=0), flip[...], preferred_element_type=jnp.float32)

    def gather(layer, which, row, src):
        for u in range(2):
            accs = [[None] * SEQ for _ in range(STEPS)]
            after = None
            for m in spans:
                even = h_ref[layer, which, pl.ds(row + 8 * u, 8), LANES * (tiles - 1 - m):LANES * (tiles - m)]
                rolled = pltpu.roll(even, LANES - 1, 1)
                odd = rolled if after is None else jnp.where(lane8 < LANES - 1, rolled, after)
                after = rolled
                for b in range(SEQ):
                    base = 16 * (SEQ * (m + 1) + b) + 8 * u
                    for two in range(2):
                        value = src[base:base + 8, LANES * two:LANES * (two + 1)]
                        for one, taps in enumerate((even, odd)):
                            part = taps * value
                            j = 2 * two + one
                            accs[j][b] = part if accs[j][b] is None else accs[j][b] + part
            for j in range(STEPS):
                for b in range(SEQ):
                    n = SEQ * j + b
                    acc[which, pl.ds(row + 8 * u, 8), LANES * n:LANES * (n + 1)] = accs[j][b]

    def close(row):
        out = jnp.zeros((16, LANES), jnp.float32)
        for which in range(2):
            for j in range(STEPS):
                for b in range(SEQ):
                    n = SEQ * j + b
                    part = jnp.sum(acc[which, pl.ds(row, 16), LANES * n:LANES * (n + 1)], axis=1, keepdims=True)
                    out = jnp.where(lane16 == (2 * b + which) * STEPS + j, part, out)
        total[pl.ds(row, 16), :] = out

    def row_of(k):
        return k * 16 if isinstance(k, int) else pl.multiple_of(k * 16, 16)

    def conv(layer, p0, p1):
        def pair(p, _):
            k = 2 * p
            step = layer * CHUNKS + k + 2
            later, after = lax.rem(lax.div(step, CHUNKS), LAYERS), lax.rem(step, CHUNKS)
            start_ahead(layer, p)
            for copy in chunk_copies(layer, k + 1):
                copy.wait()

            @pl.when(step < LAYERS * CHUNKS)
            def _():
                for copy in chunk_copies(later, after):
                    copy.wait()

            @pl.when(has_rows)
            def _():
                r0, r1, r2 = row_of(k), row_of(k + 1), row_of(after)
                turn(v_ref, layer, r1, v_odd)
                gather(layer, 0, r0, v_even)
                turn(z_ref, layer, r1, z_odd)
                gather(layer, 1, r0, z_even)
                turn(v_ref, later, r2, v_even)
                gather(layer, 0, r1, v_odd)
                turn(z_ref, later, r2, z_even)
                gather(layer, 1, r1, z_odd)

            return 0

        lax.fori_loop(p0, p1, pair, 0)

    lane_c = lax.broadcasted_iota(jnp.int32, (chan, LANES), 1)

    def hist_copy(layer, seq):
        return pltpu.make_async_remote_copy(hx.at[layer, sp, seq], hx.at[layer, sp, seq], hsend.at[layer, seq], hrecv.at[layer, sp],
                                            device_id={"sp": 2 * seq + 1}, device_id_type=MESH)

    def send_hist(layer):
        for row in range(0, chan, 16):
            close(row)
        turned = jnp.transpose(total[...])
        for b in range(SEQ):
            hx[layer, sp, b] = turned[2 * STEPS * b:2 * STEPS * (b + 1)]
        hist_copy(layer, 1).start()

        @pl.when(sp != 1)
        def _():
            hist_copy(layer, 0).start()

    def sum_hist(layer):
        for src in range(3):
            @pl.when(sp != src)
            def _():
                pltpu.make_async_remote_copy(hx.at[layer, src, own], hx.at[layer, src, own], hsend.at[layer, 0], hrecv.at[layer, src],
                                             device_id=block_peers[0], device_id_type=MESH).wait_recv()
        return (hx[layer, 0, own] + hx[layer, 1, own]) + hx[layer, 2, own]

    def sum_copies(n):
        return [pltpu.make_async_remote_copy(ar.at[n, tp], ar.at[n, tp], asend.at[n, d], arecv.at[n, tp],
                                             device_id=peers[d], device_id_type=MESH) for d in range(3)]

    def send_sum(n, part):
        ar[n, tp] = part
        for copy in sum_copies(n):
            copy.start()

    def take_sum(n):
        for d in (1, 2, 3):
            src = lax.rem(tp + d, 4)
            pltpu.make_async_remote_copy(ar.at[n, src], ar.at[n, src], asend.at[n, 0], arecv.at[n, src],
                                         device_id=peers[0], device_id_type=MESH).wait_recv()
        return ((ar[n, 0] + ar[n, 1]) + ar[n, 2]) + ar[n, 3]

    def row_copy(layer, seq, d):
        return pltpu.make_async_remote_copy(xb.at[layer, seq], xb.at[layer, seq], xsend.at[layer, d], xrecv.at[layer, seq],
                                            device_id=block_peers[d], device_id_type=MESH)

    def row_copies(layer, seq):
        return [row_copy(layer, seq, d) for d in range(3)]

    def last_copy(seq, d):
        return pltpu.make_async_remote_copy(fin.at[seq], fin.at[seq], fsend.at[d], frecv.at[seq],
                                            device_id=block_peers[d], device_id_type=MESH)

    def last_copies(seq):
        return [last_copy(seq, d) for d in range(3)]

    def project(layer, hidden):
        normed = layer_norm(hidden).astype(jnp.bfloat16)
        mixed = []
        for g in range(3):
            p = lax.dot_general(normed, win[layer, g], (((1,), (1,)), ((), ())), preferred_element_type=jnp.float32)
            p = (p + bin_ref[g, layer][None]).astype(jnp.bfloat16).astype(jnp.float32)
            prow[layer, g, 0:2, :] = st_ref[layer, own, g].astype(jnp.float32)
            prow[layer, g, 2:2 + STEPS, :] = p
            mixed.append(tap_ref[0, g, layer][None] * p + tap_ref[1, g, layer][None] * prow[layer, g, 1:1 + STEPS, :]
                         + tap_ref[2, g, layer][None] * prow[layer, g, 0:STEPS, :])
        return mixed

    def recent(layer, which, rows_f):
        rrow[layer, which, STEPS - 1:2 * STEPS - 1, :] = rows_f
        total = (lag[layer, which, 0:1] + skip_ref[layer, which][None]) * rows_f
        for back in range(1, STEPS):
            total = total + lag[layer, which, back:back + 1] * rrow[layer, which, STEPS - 1 - back:2 * STEPS - 1 - back, :]
        return total

    def mixer(layer, mixed, hist):
        value = mixed[2].astype(jnp.bfloat16).astype(jnp.float32)
        long_one = hist[:STEPS] + recent(layer, 0, value)
        z_rows = (mixed[0] * long_one).astype(jnp.bfloat16).astype(jnp.float32)
        long_two = hist[STEPS:] + recent(layer, 1, z_rows)
        y_rows = (mixed[1] * long_two).astype(jnp.bfloat16)
        send_sum(2 * layer, jnp.dot(y_rows, wout[layer], preferred_element_type=jnp.float32))
        for g in range(3):
            xb[layer, own, 2 * g:2 * g + 2, :] = prow[layer, g, STEPS:STEPS + 2, :]
        xb[layer, own, 6:8, :] = jnp.zeros((2, chan), jnp.float32)
        xb[layer, own, 8:8 + STEPS, :] = value
        xb[layer, own, 8 + STEPS:8 + 2 * STEPS, :] = z_rows
        for copy in row_copies(layer, own):
            copy.start()

    def mlp(layer, hidden):
        up = jnp.dot(layer_norm(hidden).astype(jnp.bfloat16), wup[layer], preferred_element_type=jnp.float32)
        return jnp.dot(jax.nn.gelu(up).astype(jnp.bfloat16), wdown[layer], preferred_element_type=jnp.float32)

    def put_rows(layer):
        for b in range(SEQ):
            @pl.when(sp != 2 * b + 1)
            def _():
                row_copy(layer, b, 0).wait_recv()

        for b in range(SEQ):
            newrow[2 * STEPS * b:2 * STEPS * (b + 1), 0:chan] = xb[layer, b, 8:16, :]
            for g in range(3):
                st_out[layer, b, g] = xb[layer, b, 2 * g:2 * g + 2, :].astype(jnp.bfloat16)
        turned = jnp.transpose(newrow[...])[:chan]

        @pl.when(sp == 3)
        def _():
            for b in range(SEQ):
                for n, cache in enumerate((v_ref, z_ref)):
                    at = STEPS * (2 * b + n)
                    moved = turned if at == 0 else pltpu.roll(turned, LANES - at, 1)
                    cache[layer, b, :, 0:LANES] = jnp.where(lane_c < STEPS, moved, 0.0).astype(jnp.bfloat16)

    newrow[...] = jnp.zeros_like(newrow)
    rrow[...] = jnp.zeros_like(rrow)
    kk = lax.broadcasted_iota(jnp.int32, flip.shape, 0)
    nn = lax.broadcasted_iota(jnp.int32, flip.shape, 1)
    flip[...] = jnp.where(kk == jnp.where(nn < LANES, LANES - nn, 2 * LANES + 2 - nn), 1.0, 0.0).astype(jnp.bfloat16)
    for copy in chunk_copies(0, 0):
        copy.wait()

    @pl.when(has_rows)
    def _():
        turn(v_ref, 0, 0, v_even)
        turn(z_ref, 0, 0, z_even)

    def stage(n, _):
        at_least = [None] + [lax.div(n + 3 - i, 3) if i == 1 else lax.div(n, i) for i in (1, 2, 3)]
        conv(at_least[1], FIRST * at_least[2] + SECOND * at_least[3],
             CHUNKS // 2 - (CHUNKS // 2 - FIRST) * (at_least[1] - at_least[2])
             - (CHUNKS // 2 - FIRST - SECOND) * (at_least[2] - at_least[3]))

        @pl.when((n == 0) & carries)
        def _():
            pl.semaphore_wait(barrier, 6)

        @pl.when((n == 0) & jnp.logical_not(carries))
        def _():
            pl.semaphore_wait(barrier, 3)

        @pl.when(((n == 0) | (n == 3)) & has_rows)
        def _():
            send_hist(lax.div(n, 3))

        @pl.when(n == 0)
        def _():
            for copy in smalls:
                copy.wait()

        @pl.when((n == 0) & carries)
        def _():
            hidden = jnp.where(own == 0, jnp.concatenate([e_ref[j].astype(jnp.float32)[0:1] for j in range(STEPS)], axis=0),
                               jnp.concatenate([e_ref[j].astype(jnp.float32)[1:2] for j in range(STEPS)], axis=0))
            held[...] = hidden
            weight_copy(0, 0).wait()
            for g, rows_f in enumerate(project(0, hidden)):
                mixed_ref[g] = rows_f
            for layer in range(LAYERS):
                for which in range(2):
                    lag[layer, which] = jnp.transpose(lag_ref[layer, which])[:8]
            for n_w in (1, 2, 3):
                weight_copy(0, n_w).wait()

        @pl.when((n == 1) & carries)
        def _():
            mixer(0, [mixed_ref[g] for g in range(3)], sum_hist(0))

        @pl.when((n == 2) & carries)
        def _():
            hidden = held[...] + take_sum(0) + bout_ref[0:1]
            send_sum(1, mlp(0, hidden))
            held[...] = hidden

        return 0

    lax.fori_loop(0, 4, stage, 0)

    @pl.when(carries)
    def _():
        weight_copy(1, 0).wait()
        hidden = held[...] + take_sum(1)
        mixed = project(1, hidden)
        weight_copy(1, 1).wait()
        mixer(1, mixed, sum_hist(1))
        put_rows(0)
        weight_copy(1, 2).wait()
        weight_copy(1, 3).wait()
        hidden = hidden + take_sum(2) + bout_ref[1:2]
        send_sum(3, mlp(1, hidden))
        put_rows(1)
        fin[own] = hidden + take_sum(3)
        for copy in last_copies(own):
            copy.start()
        for layer in range(LAYERS):
            for copy in row_copies(layer, own):
                copy.wait_send()
        for n in range(4):
            for copy in sum_copies(n):
                copy.wait_send()
        for copy in last_copies(own):
            copy.wait_send()

    @pl.when(jnp.logical_not(carries))
    def _():
        put_rows(0)
        put_rows(1)

    for layer in range(LAYERS):
        @pl.when(has_rows)
        def _():
            hist_copy(layer, 1).wait_send()

            @pl.when(sp != 1)
            def _():
                hist_copy(layer, 0).wait_send()

    for b in range(SEQ):
        @pl.when(sp != 2 * b + 1)
        def _():
            last_copy(b, 0).wait_recv()

        for j in range(STEPS):
            hid_out[j, b:b + 1, :] = fin[b, j:j + 1, :]


def emit(hid, v, z, st, hid_o, v_o, z_o, st_o, sem):
    copies = []
    for layer in range(LAYERS):
        for b in range(SEQ):
            for part in range(2):
                rows = pl.ds(part * v.shape[2] // 2, v.shape[2] // 2)
                copies += [(v.at[layer, b, rows], v_o.at[layer, b, rows]), (z.at[layer, b, rows], z_o.at[layer, b, rows])]
    copies = [(hid, hid_o), (st, st_o)] + copies
    copies = [pltpu.make_async_copy(src, dst, sem.at[n]) for n, (src, dst) in enumerate(copies)]
    for copy in copies:
        copy.start()
    for copy in copies:
        copy.wait()


def solution(mesh):
    def device_fn(step_emb, v_cache, z_cache, short_state, w_in, b_in, short_taps, long_filt, skip_gain, w_out, b_out, w_up, w_down):
        chan = v_cache.shape[3]
        shard_len = v_cache.shape[2]
        model = step_emb.shape[2]
        args = (
            step_emb,
            jnp.swapaxes(v_cache, 2, 3),
            jnp.swapaxes(z_cache, 2, 3),
            jnp.transpose(short_state, (0, 1, 3, 2, 4)),
            jnp.transpose(w_in, (0, 2, 3, 1)),
            jnp.transpose(b_in, (1, 0, 2)),
            jnp.transpose(short_taps, (1, 2, 0, 3)),
            jnp.swapaxes(long_filt, 2, 3),
            skip_gain,
            w_out,
            b_out,
            w_up,
            w_down,
        )
        args = tuple(pltpu.with_memory_space_constraint(arg, pltpu.HBM) for arg in args)
        f32, bf16 = jnp.float32, jnp.bfloat16
        dma = pltpu.SemaphoreType.DMA
        hid, v_out, z_out, st_out = pl.pallas_call(
            kernel,
            out_shape=(
                jax.ShapeDtypeStruct(step_emb.shape, f32),
                pltpu.VMEM(args[1].shape, bf16),
                pltpu.VMEM(args[2].shape, bf16),
                jax.ShapeDtypeStruct(args[3].shape, bf16),
            ),
            in_specs=[pl.BlockSpec(memory_space=pltpu.HBM)] * 13,
            out_specs=[pl.BlockSpec(memory_space=pltpu.VMEM)] * 4,
            scratch_shapes=[
                pltpu.VMEM(step_emb.shape, bf16),
                pltpu.VMEM(args[3].shape, bf16),
                pltpu.VMEM(args[4].shape, bf16),
                pltpu.VMEM(args[5].shape, f32),
                pltpu.VMEM(args[6].shape, f32),
                pltpu.VMEM((LAYERS, 2, chan, shard_len + LANES), f32),
                pltpu.VMEM((LAYERS, 2, chan, LANES), f32),
                pltpu.VMEM(skip_gain.shape, f32),
                pltpu.VMEM(w_out.shape, bf16),
                pltpu.VMEM(b_out.shape, f32),
                pltpu.VMEM(w_up.shape, bf16),
                pltpu.VMEM(w_down.shape, bf16),
                pltpu.VMEM((2 * LANES, 2 * LANES), bf16),
                *[pltpu.VMEM((16 * SEQ * (shard_len // LANES + 1), 2 * LANES), f32)] * 4,
                pltpu.VMEM((2, chan, ROWS * LANES), f32),
                pltpu.VMEM((chan, LANES), f32),
                pltpu.VMEM((LAYERS, 2, 8, chan), f32),
                pltpu.VMEM((LAYERS, 3, 8, chan), f32),
                pltpu.VMEM((LAYERS, 2, 8, chan), f32),
                pltpu.VMEM((LANES, 2 * LANES), f32),
                pltpu.VMEM((LAYERS, 4, SEQ, 2 * STEPS, chan), f32),
                pltpu.VMEM((4, 4, STEPS, model), f32),
                pltpu.VMEM((LAYERS, SEQ, 16, chan), f32),
                pltpu.VMEM((SEQ, STEPS, model), f32),
                pltpu.VMEM((STEPS, model), f32),
                pltpu.VMEM((3, STEPS, chan), f32),
                dma((7,)),
                dma((LAYERS, CHUNKS, 3)),
                dma((LAYERS, 4)),
                dma((LAYERS, SEQ)),
                dma((LAYERS, 4)),
                dma((4, 3)),
                dma((4, 4)),
                dma((LAYERS, 3)),
                dma((LAYERS, SEQ)),
                dma((3,)),
                dma((SEQ,)),
            ],
            compiler_params=pltpu.CompilerParams(collective_id=0, has_side_effects=True, vmem_limit_bytes=40 * 1024 * 1024),
            name="decode",
        )(*args)
        hid, v_out, z_out, st_out = pl.pallas_call(
            emit,
            out_shape=(
                jax.ShapeDtypeStruct(hid.shape, f32),
                jax.ShapeDtypeStruct(v_out.shape, bf16),
                jax.ShapeDtypeStruct(z_out.shape, bf16),
                jax.ShapeDtypeStruct(st_out.shape, bf16),
            ),
            in_specs=[pl.BlockSpec(memory_space=pltpu.VMEM)] * 4,
            out_specs=[pl.BlockSpec(memory_space=pltpu.HBM)] * 4,
            scratch_shapes=[dma((8 * LAYERS + 2,))],
            compiler_params=pltpu.CompilerParams(vmem_limit_bytes=1024 * 1024),
            name="emit",
        )(hid, v_out, z_out, st_out)
        return (hid, jnp.swapaxes(v_out, 2, 3), jnp.swapaxes(z_out, 2, 3), jnp.transpose(st_out, (0, 1, 3, 2, 4)))

    specs_in = (
        P(None, "dp", None),
        P(None, "dp", "sp", "tp"),
        P(None, "dp", "sp", "tp"),
        P(None, "dp", None, None, "tp"),
        P(None, None, None, "tp"),
        P(None, None, "tp"),
        P(None, None, None, "tp"),
        P(None, None, None, "tp"),
        P(None, None, "tp"),
        P(None, "tp", None),
        P(None, None),
        P(None, None, "tp"),
        P(None, "tp", None),
    )
    specs_out = (
        P(None, "dp", None),
        P(None, "dp", "sp", "tp"),
        P(None, "dp", "sp", "tp"),
        P(None, "dp", None, None, "tp"),
    )
    return jax.shard_map(device_fn, mesh=mesh, in_specs=specs_in, out_specs=specs_out, check_vma=False)
```

```python
import functools

import jax
import jax.numpy as jnp
from jax import lax
from jax.experimental import pallas as pl
from jax.experimental.pallas import tpu as pltpu
from jax.sharding import PartitionSpec as P

STEPS = 4
LAYERS = 2
SEQ = 2
ROWS = STEPS * SEQ
LANES = 128
CHUNKS = 12
FIRST, SECOND = 2, 3
MESH = pl.DeviceIdType.MESH


def layer_norm(rows_in):
    mean_val = jnp.mean(rows_in, axis=-1, keepdims=True)
    centered = rows_in - mean_val
    var_val = jnp.mean(centered * centered, axis=-1, keepdims=True)
    return centered * lax.rsqrt(var_val + 1e-5)


def kernel(e_hbm, v_hbm, z_hbm, st_hbm, win_hbm, bin_hbm, tap_hbm, h_hbm, skip_hbm, wout_hbm, bout_hbm, wup_hbm, wdown_hbm,
           hid_out, v_ref, z_ref, st_out,
           e_ref, st_ref, win, bin_ref, tap_ref, h_ref, lag_ref, skip_ref, wout, bout_ref, wup, wdown,
           flip, v_even, z_even, v_odd, z_odd, acc, total, lag, prow, rrow, newrow, hx, ar, xb, fin, held, mixed_ref,
           small_sem, chunk_sem, w_sem, hsend, hrecv, asend, arecv, xsend, xrecv, fsend, frecv):
    tp = lax.axis_index("tp")
    sp = lax.axis_index("sp")
    own = lax.div(sp, 2)
    carries = lax.rem(sp, 2) == 1
    has_rows = sp != 3
    chan, shard_len = v_hbm.shape[2], v_hbm.shape[3]
    model = e_hbm.shape[2]
    tiles = shard_len // LANES
    rows_per = chan // CHUNKS
    half = lax.div(tp, 2)
    near = tp + 1 - 2 * lax.rem(tp, 2)
    peers = [{"tp": 3 - 3 * half}, {"tp": 2 - half}, {"tp": near}]
    block_peers = [{"sp": lax.rem(sp + d, 4)} for d in (2, 3, 1)]

    barrier = pltpu.get_barrier_semaphore()
    for peer in block_peers:
        pl.semaphore_signal(barrier, inc=1, device_id=peer, device_id_type=MESH)

    @pl.when(carries)
    def _():
        for peer in peers:
            pl.semaphore_signal(barrier, inc=1, device_id=peer, device_id_type=MESH)

    smalls = [pltpu.make_async_copy(src, dst, small_sem.at[n]) for n, (src, dst) in enumerate((
        (e_hbm, e_ref), (st_hbm, st_ref), (bin_hbm, bin_ref), (tap_hbm, tap_ref), (skip_hbm, skip_ref), (bout_hbm, bout_ref),
        (h_hbm.at[:, :, :, pl.ds(0, LANES)], lag_ref)))]
    first = pl.multiple_of(lax.rem(5 - sp, 3) * shard_len, LANES)

    def chunk_copies(layer, k):
        rows = pl.ds(k * rows_per if isinstance(k, int) else pl.multiple_of(k * rows_per, rows_per), rows_per)
        return [
            pltpu.make_async_copy(v_hbm.at[layer, :, rows, :], v_ref.at[layer, :, rows, :], chunk_sem.at[layer, k, 0]),
            pltpu.make_async_copy(z_hbm.at[layer, :, rows, :], z_ref.at[layer, :, rows, :], chunk_sem.at[layer, k, 1]),
            pltpu.make_async_copy(h_hbm.at[layer, :, rows, pl.ds(first, shard_len + LANES)], h_ref.at[layer, :, rows, :],
                                  chunk_sem.at[layer, k, 2]),
        ]

    def weight_copy(layer, n):
        src, dst = ((win_hbm, win), (wout_hbm, wout), (wup_hbm, wup), (wdown_hbm, wdown))[n]
        return pltpu.make_async_copy(src.at[layer], dst.at[layer], w_sem.at[layer, n])

    def start_weights(layer):
        @pl.when(carries)
        def _():
            for n in range(4):
                weight_copy(layer, n).start()

    for n in range(LAYERS * CHUNKS):
        layer, k = divmod(n, CHUNKS)
        for copy in chunk_copies(layer, k):
            copy.start()
        if n == CHUNKS:
            for copy in smalls:
                copy.start()
            start_weights(0)
    start_weights(1)

    lane8 = lax.broadcasted_iota(jnp.int32, (8, LANES), 1)
    lane16 = lax.broadcasted_iota(jnp.int32, (16, LANES), 1)
    spans = range(-1, tiles)

    def turn(cache, layer, row, dst):
        zero = jnp.zeros((16, LANES), jnp.bfloat16)

        def values(b, m):
            return cache[layer, b, pl.ds(row, 16), LANES * m:LANES * (m + 1)] if 0 <= m < tiles else zero

        parts = [jnp.concatenate([values(b, m), values(b, m + 1)], axis=1) for m in spans for b in range(SEQ)]
        dst[...] = jnp.dot(jnp.concatenate(parts, axis=0), flip[...], preferred_element_type=jnp.float32)

    def gather(layer, which, row, src):
        for u in range(2):
            accs = [[None] * SEQ for _ in range(STEPS)]
            after = None
            for m in spans:
                even = h_ref[layer, which, pl.ds(row + 8 * u, 8), LANES * (tiles - 1 - m):LANES * (tiles - m)]
                rolled = pltpu.roll(even, LANES - 1, 1)
                odd = rolled if after is None else jnp.where(lane8 < LANES - 1, rolled, after)
                after = rolled
                for b in range(SEQ):
                    base = 16 * (SEQ * (m + 1) + b) + 8 * u
                    for two in range(2):
                        value = src[base:base + 8, LANES * two:LANES * (two + 1)]
                        for one, taps in enumerate((even, odd)):
                            part = taps * value
                            j = 2 * two + one
                            accs[j][b] = part if accs[j][b] is None else accs[j][b] + part
            for j in range(STEPS):
                for b in range(SEQ):
                    n = SEQ * j + b
                    acc[which, pl.ds(row + 8 * u, 8), LANES * n:LANES * (n + 1)] = accs[j][b]

    def close(row):
        out = jnp.zeros((16, LANES), jnp.float32)
        for which in range(2):
            for j in range(STEPS):
                for b in range(SEQ):
                    n = SEQ * j + b
                    part = jnp.sum(acc[which, pl.ds(row, 16), LANES * n:LANES * (n + 1)], axis=1, keepdims=True)
                    out = jnp.where(lane16 == (2 * b + which) * STEPS + j, part, out)
        total[pl.ds(row, 16), :] = out

    def row_of(k):
        return k * 16 if isinstance(k, int) else pl.multiple_of(k * 16, 16)

    def conv(layer, p0, p1):
        def pair(p, _):
            k = 2 * p
            step = layer * CHUNKS + k + 2
            later, after = lax.rem(lax.div(step, CHUNKS), LAYERS), lax.rem(step, CHUNKS)
            for copy in chunk_copies(layer, k + 1):
                copy.wait()

            @pl.when(step < LAYERS * CHUNKS)
            def _():
                for copy in chunk_copies(later, after):
                    copy.wait()

            @pl.when(has_rows)
            def _():
                r0, r1, r2 = row_of(k), row_of(k + 1), row_of(after)
                turn(v_ref, layer, r1, v_odd)
                gather(layer, 0, r0, v_even)
                turn(z_ref, layer, r1, z_odd)
                gather(layer, 1, r0, z_even)
                turn(v_ref, later, r2, v_even)
                gather(layer, 0, r1, v_odd)
                turn(z_ref, later, r2, z_even)
                gather(layer, 1, r1, z_odd)

            return 0

        lax.fori_loop(p0, p1, pair, 0)

    lane_c = lax.broadcasted_iota(jnp.int32, (chan, LANES), 1)

    def hist_copy(layer, seq):
        return pltpu.make_async_remote_copy(hx.at[layer, sp, seq], hx.at[layer, sp, seq], hsend.at[layer, seq], hrecv.at[layer, sp],
                                            device_id={"sp": 2 * seq + 1}, device_id_type=MESH)

    def send_hist(layer):
        for row in range(0, chan, 16):
            close(row)
        turned = jnp.transpose(total[...])
        for b in range(SEQ):
            hx[layer, sp, b] = turned[2 * STEPS * b:2 * STEPS * (b + 1)]
        hist_copy(layer, 1).start()

        @pl.when(sp != 1)
        def _():
            hist_copy(layer, 0).start()

    def sum_hist(layer):
        for src in range(3):
            @pl.when(sp != src)
            def _():
                pltpu.make_async_remote_copy(hx.at[layer, src, own], hx.at[layer, src, own], hsend.at[layer, 0], hrecv.at[layer, src],
                                             device_id=block_peers[0], device_id_type=MESH).wait_recv()
        return (hx[layer, 0, own] + hx[layer, 1, own]) + hx[layer, 2, own]

    def sum_copies(n):
        return [pltpu.make_async_remote_copy(ar.at[n, tp], ar.at[n, tp], asend.at[n, d], arecv.at[n, tp],
                                             device_id=peers[d], device_id_type=MESH) for d in range(3)]

    def send_sum(n, part):
        ar[n, tp] = part
        for copy in sum_copies(n):
            copy.start()

    def take_sum(n):
        for d in (1, 2, 3):
            src = lax.rem(tp + d, 4)
            pltpu.make_async_remote_copy(ar.at[n, src], ar.at[n, src], asend.at[n, 0], arecv.at[n, src],
                                         device_id=peers[0], device_id_type=MESH).wait_recv()
        return ((ar[n, 0] + ar[n, 1]) + ar[n, 2]) + ar[n, 3]

    def row_copy(layer, seq, d):
        return pltpu.make_async_remote_copy(xb.at[layer, seq], xb.at[layer, seq], xsend.at[layer, d], xrecv.at[layer, seq],
                                            device_id=block_peers[d], device_id_type=MESH)

    def row_copies(layer, seq):
        return [row_copy(layer, seq, d) for d in range(3)]

    def last_copy(seq, d):
        return pltpu.make_async_remote_copy(fin.at[seq], fin.at[seq], fsend.at[d], frecv.at[seq],
                                            device_id=block_peers[d], device_id_type=MESH)

    def last_copies(seq):
        return [last_copy(seq, d) for d in range(3)]

    def project(layer, hidden):
        normed = layer_norm(hidden).astype(jnp.bfloat16)
        mixed = []
        for g in range(3):
            p = lax.dot_general(normed, win[layer, g], (((1,), (1,)), ((), ())), preferred_element_type=jnp.float32)
            p = (p + bin_ref[g, layer][None]).astype(jnp.bfloat16).astype(jnp.float32)
            prow[layer, g, 0:2, :] = st_ref[layer, own, g].astype(jnp.float32)
            prow[layer, g, 2:2 + STEPS, :] = p
            mixed.append(tap_ref[0, g, layer][None] * p + tap_ref[1, g, layer][None] * prow[layer, g, 1:1 + STEPS, :]
                         + tap_ref[2, g, layer][None] * prow[layer, g, 0:STEPS, :])
        return mixed

    def recent(layer, which, rows_f):
        rrow[layer, which, STEPS - 1:2 * STEPS - 1, :] = rows_f
        total = (lag[layer, which, 0:1] + skip_ref[layer, which][None]) * rows_f
        for back in range(1, STEPS):
            total = total + lag[layer, which, back:back + 1] * rrow[layer, which, STEPS - 1 - back:2 * STEPS - 1 - back, :]
        return total

    def mixer(layer, mixed, hist):
        value = mixed[2].astype(jnp.bfloat16).astype(jnp.float32)
        long_one = hist[:STEPS] + recent(layer, 0, value)
        z_rows = (mixed[0] * long_one).astype(jnp.bfloat16).astype(jnp.float32)
        long_two = hist[STEPS:] + recent(layer, 1, z_rows)
        y_rows = (mixed[1] * long_two).astype(jnp.bfloat16)
        send_sum(2 * layer, jnp.dot(y_rows, wout[layer], preferred_element_type=jnp.float32))
        for g in range(3):
            xb[layer, own, 2 * g:2 * g + 2, :] = prow[layer, g, STEPS:STEPS + 2, :]
        xb[layer, own, 6:8, :] = jnp.zeros((2, chan), jnp.float32)
        xb[layer, own, 8:8 + STEPS, :] = value
        xb[layer, own, 8 + STEPS:8 + 2 * STEPS, :] = z_rows
        for copy in row_copies(layer, own):
            copy.start()

    def mlp(layer, hidden):
        up = jnp.dot(layer_norm(hidden).astype(jnp.bfloat16), wup[layer], preferred_element_type=jnp.float32)
        return jnp.dot(jax.nn.gelu(up).astype(jnp.bfloat16), wdown[layer], preferred_element_type=jnp.float32)

    def put_rows(layer):
        for b in range(SEQ):
            @pl.when(sp != 2 * b + 1)
            def _():
                row_copy(layer, b, 0).wait_recv()

        for b in range(SEQ):
            newrow[2 * STEPS * b:2 * STEPS * (b + 1), 0:chan] = xb[layer, b, 8:16, :]
            for g in range(3):
                st_out[layer, b, g] = xb[layer, b, 2 * g:2 * g + 2, :].astype(jnp.bfloat16)
        turned = jnp.transpose(newrow[...])[:chan]

        @pl.when(sp == 3)
        def _():
            for b in range(SEQ):
                for n, cache in enumerate((v_ref, z_ref)):
                    at = STEPS * (2 * b + n)
                    moved = turned if at == 0 else pltpu.roll(turned, LANES - at, 1)
                    cache[layer, b, :, 0:LANES] = jnp.where(lane_c < STEPS, moved, 0.0).astype(jnp.bfloat16)

    newrow[...] = jnp.zeros_like(newrow)
    rrow[...] = jnp.zeros_like(rrow)
    kk = lax.broadcasted_iota(jnp.int32, flip.shape, 0)
    nn = lax.broadcasted_iota(jnp.int32, flip.shape, 1)
    flip[...] = jnp.where(kk == jnp.where(nn < LANES, LANES - nn, 2 * LANES + 2 - nn), 1.0, 0.0).astype(jnp.bfloat16)
    head = chunk_copies(0, 0)
    head[0].wait()
    head[1].wait()

    @pl.when(has_rows)
    def _():
        turn(v_ref, 0, 0, v_even)
        turn(z_ref, 0, 0, z_even)

    head[2].wait()

    def stage(n, _):
        at_least = [None] + [lax.div(n + 3 - i, 3) if i == 1 else lax.div(n, i) for i in (1, 2, 3)]
        conv(at_least[1], FIRST * at_least[2] + SECOND * at_least[3],
             CHUNKS // 2 - (CHUNKS // 2 - FIRST) * (at_least[1] - at_least[2])
             - (CHUNKS // 2 - FIRST - SECOND) * (at_least[2] - at_least[3]))

        @pl.when((n == 0) & carries)
        def _():
            pl.semaphore_wait(barrier, 6)

        @pl.when((n == 0) & jnp.logical_not(carries))
        def _():
            pl.semaphore_wait(barrier, 3)

        @pl.when(((n == 0) | (n == 3)) & has_rows)
        def _():
            send_hist(lax.div(n, 3))

        @pl.when(n == 0)
        def _():
            for copy in smalls:
                copy.wait()

        @pl.when((n == 0) & carries)
        def _():
            hidden = jnp.where(own == 0, jnp.concatenate([e_ref[j].astype(jnp.float32)[0:1] for j in range(STEPS)], axis=0),
                               jnp.concatenate([e_ref[j].astype(jnp.float32)[1:2] for j in range(STEPS)], axis=0))
            held[...] = hidden
            weight_copy(0, 0).wait()
            for g, rows_f in enumerate(project(0, hidden)):
                mixed_ref[g] = rows_f
            for layer in range(LAYERS):
                for which in range(2):
                    lag[layer, which] = jnp.transpose(lag_ref[layer, which])[:8]
            for n_w in (1, 2, 3):
                weight_copy(0, n_w).wait()

        @pl.when((n == 1) & carries)
        def _():
            mixer(0, [mixed_ref[g] for g in range(3)], sum_hist(0))

        @pl.when((n == 2) & carries)
        def _():
            hidden = held[...] + take_sum(0) + bout_ref[0:1]
            send_sum(1, mlp(0, hidden))
            held[...] = hidden

        return 0

    lax.fori_loop(0, 4, stage, 0)

    @pl.when(carries)
    def _():
        weight_copy(1, 0).wait()
        hidden = held[...] + take_sum(1)
        mixed = project(1, hidden)
        weight_copy(1, 1).wait()
        mixer(1, mixed, sum_hist(1))
        put_rows(0)
        weight_copy(1, 2).wait()
        weight_copy(1, 3).wait()
        hidden = hidden + take_sum(2) + bout_ref[1:2]
        send_sum(3, mlp(1, hidden))
        put_rows(1)
        fin[own] = hidden + take_sum(3)
        for copy in last_copies(own):
            copy.start()
        for layer in range(LAYERS):
            for copy in row_copies(layer, own):
                copy.wait_send()
        for n in range(4):
            for copy in sum_copies(n):
                copy.wait_send()
        for copy in last_copies(own):
            copy.wait_send()

    @pl.when(jnp.logical_not(carries))
    def _():
        put_rows(0)
        put_rows(1)

    for layer in range(LAYERS):
        @pl.when(has_rows)
        def _():
            hist_copy(layer, 1).wait_send()

            @pl.when(sp != 1)
            def _():
                hist_copy(layer, 0).wait_send()

    for b in range(SEQ):
        @pl.when(sp != 2 * b + 1)
        def _():
            last_copy(b, 0).wait_recv()

        for j in range(STEPS):
            hid_out[j, b:b + 1, :] = fin[b, j:j + 1, :]


def emit(hid, v, z, st, hid_o, v_o, z_o, st_o, sem):
    copies = []
    for layer in range(LAYERS):
        for b in range(SEQ):
            copies += [(v.at[layer, b], v_o.at[layer, b]), (z.at[layer, b], z_o.at[layer, b])]
    copies += [(hid, hid_o), (st, st_o)]
    copies = [pltpu.make_async_copy(src, dst, sem.at[n]) for n, (src, dst) in enumerate(copies)]
    for copy in copies:
        copy.start()
    for copy in copies:
        copy.wait()


def solution(mesh):
    def device_fn(step_emb, v_cache, z_cache, short_state, w_in, b_in, short_taps, long_filt, skip_gain, w_out, b_out, w_up, w_down):
        chan = v_cache.shape[3]
        shard_len = v_cache.shape[2]
        model = step_emb.shape[2]
        args = (
            step_emb,
            jnp.swapaxes(v_cache, 2, 3),
            jnp.swapaxes(z_cache, 2, 3),
            jnp.transpose(short_state, (0, 1, 3, 2, 4)),
            jnp.transpose(w_in, (0, 2, 3, 1)),
            jnp.transpose(b_in, (1, 0, 2)),
            jnp.transpose(short_taps, (1, 2, 0, 3)),
            jnp.swapaxes(long_filt, 2, 3),
            skip_gain,
            w_out,
            b_out,
            w_up,
            w_down,
        )
        args = tuple(pltpu.with_memory_space_constraint(arg, pltpu.HBM) for arg in args)
        f32, bf16 = jnp.float32, jnp.bfloat16
        dma = pltpu.SemaphoreType.DMA
        hid, v_out, z_out, st_out = pl.pallas_call(
            kernel,
            out_shape=(
                jax.ShapeDtypeStruct(step_emb.shape, f32),
                pltpu.VMEM(args[1].shape, bf16),
                pltpu.VMEM(args[2].shape, bf16),
                jax.ShapeDtypeStruct(args[3].shape, bf16),
            ),
            in_specs=[pl.BlockSpec(memory_space=pltpu.HBM)] * 13,
            out_specs=[pl.BlockSpec(memory_space=pltpu.VMEM)] * 4,
            scratch_shapes=[
                pltpu.VMEM(step_emb.shape, bf16),
                pltpu.VMEM(args[3].shape, bf16),
                pltpu.VMEM(args[4].shape, bf16),
                pltpu.VMEM(args[5].shape, f32),
                pltpu.VMEM(args[6].shape, f32),
                pltpu.VMEM((LAYERS, 2, chan, shard_len + LANES), f32),
                pltpu.VMEM((LAYERS, 2, chan, LANES), f32),
                pltpu.VMEM(skip_gain.shape, f32),
                pltpu.VMEM(w_out.shape, bf16),
                pltpu.VMEM(b_out.shape, f32),
                pltpu.VMEM(w_up.shape, bf16),
                pltpu.VMEM(w_down.shape, bf16),
                pltpu.VMEM((2 * LANES, 2 * LANES), bf16),
                *[pltpu.VMEM((16 * SEQ * (shard_len // LANES + 1), 2 * LANES), f32)] * 4,
                pltpu.VMEM((2, chan, ROWS * LANES), f32),
                pltpu.VMEM((chan, LANES), f32),
                pltpu.VMEM((LAYERS, 2, 8, chan), f32),
                pltpu.VMEM((LAYERS, 3, 8, chan), f32),
                pltpu.VMEM((LAYERS, 2, 8, chan), f32),
                pltpu.VMEM((LANES, 2 * LANES), f32),
                pltpu.VMEM((LAYERS, 4, SEQ, 2 * STEPS, chan), f32),
                pltpu.VMEM((4, 4, STEPS, model), f32),
                pltpu.VMEM((LAYERS, SEQ, 16, chan), f32),
                pltpu.VMEM((SEQ, STEPS, model), f32),
                pltpu.VMEM((STEPS, model), f32),
                pltpu.VMEM((3, STEPS, chan), f32),
                dma((7,)),
                dma((LAYERS, CHUNKS, 3)),
                dma((LAYERS, 4)),
                dma((LAYERS, SEQ)),
                dma((LAYERS, 4)),
                dma((4, 3)),
                dma((4, 4)),
                dma((LAYERS, 3)),
                dma((LAYERS, SEQ)),
                dma((3,)),
                dma((SEQ,)),
            ],
            compiler_params=pltpu.CompilerParams(collective_id=0, has_side_effects=True, vmem_limit_bytes=40 * 1024 * 1024),
            name="decode",
        )(*args)
        hid, v_out, z_out, st_out = pl.pallas_call(
            emit,
            out_shape=(
                jax.ShapeDtypeStruct(hid.shape, f32),
                jax.ShapeDtypeStruct(v_out.shape, bf16),
                jax.ShapeDtypeStruct(z_out.shape, bf16),
                jax.ShapeDtypeStruct(st_out.shape, bf16),
            ),
            in_specs=[pl.BlockSpec(memory_space=pltpu.VMEM)] * 4,
            out_specs=[pl.BlockSpec(memory_space=pltpu.HBM)] * 4,
            scratch_shapes=[dma((4 * LAYERS + 2,))],
            compiler_params=pltpu.CompilerParams(vmem_limit_bytes=1024 * 1024),
            name="emit",
        )(hid, v_out, z_out, st_out)
        return (hid, jnp.swapaxes(v_out, 2, 3), jnp.swapaxes(z_out, 2, 3), jnp.transpose(st_out, (0, 1, 3, 2, 4)))

    specs_in = (
        P(None, "dp", None),
        P(None, "dp", "sp", "tp"),
        P(None, "dp", "sp", "tp"),
        P(None, "dp", None, None, "tp"),
        P(None, None, None, "tp"),
        P(None, None, "tp"),
        P(None, None, None, "tp"),
        P(None, None, None, "tp"),
        P(None, None, "tp"),
        P(None, "tp", None),
        P(None, None),
        P(None, None, "tp"),
        P(None, "tp", None),
    )
    specs_out = (
        P(None, "dp", None),
        P(None, "dp", "sp", "tp"),
        P(None, "dp", "sp", "tp"),
        P(None, "dp", None, None, "tp"),
    )
    return jax.shard_map(device_fn, mesh=mesh, in_specs=specs_in, out_specs=specs_out, check_vma=False)
```

```python
import functools

import jax
import jax.numpy as jnp
from jax import lax
from jax.experimental import pallas as pl
from jax.experimental.pallas import tpu as pltpu
from jax.sharding import PartitionSpec as P

STEPS = 4
LAYERS = 2
SEQ = 2
ROWS = STEPS * SEQ
LANES = 128
CHUNKS = 12
FIRST, SECOND = 2, 3
MESH = pl.DeviceIdType.MESH


def layer_norm(rows_in):
    mean_val = jnp.mean(rows_in, axis=-1, keepdims=True)
    centered = rows_in - mean_val
    var_val = jnp.mean(centered * centered, axis=-1, keepdims=True)
    return centered * lax.rsqrt(var_val + 1e-5)


def kernel(e_hbm, v_hbm, z_hbm, st_hbm, win_hbm, bin_hbm, tap_hbm, h_hbm, skip_hbm, wout_hbm, bout_hbm, wup_hbm, wdown_hbm,
           hid_out, v_ref, z_ref, st_out,
           e_ref, st_ref, win, bin_ref, tap_ref, h_ref, lag_ref, skip_ref, wout, bout_ref, wup, wdown,
           flip, v_even, z_even, v_odd, z_odd, acc, total, lag, prow, rrow, newrow, hx, ar, xb, fin, held, mixed_ref,
           small_sem, chunk_sem, w_sem, hsend, hrecv, asend, arecv, xsend, xrecv, fsend, frecv):
    tp = lax.axis_index("tp")
    sp = lax.axis_index("sp")
    own = lax.div(sp, 2)
    carries = lax.rem(sp, 2) == 1
    has_rows = sp != 3
    chan, shard_len = v_hbm.shape[2], v_hbm.shape[3]
    model = e_hbm.shape[2]
    tiles = shard_len // LANES
    rows_per = chan // CHUNKS
    half = lax.div(tp, 2)
    near = tp + 1 - 2 * lax.rem(tp, 2)
    peers = [{"tp": 3 - 3 * half}, {"tp": 2 - half}, {"tp": near}]
    block_peers = [{"sp": lax.rem(sp + d, 4)} for d in (2, 3, 1)]

    barrier = pltpu.get_barrier_semaphore()
    for peer in block_peers:
        pl.semaphore_signal(barrier, inc=1, device_id=peer, device_id_type=MESH)

    @pl.when(carries)
    def _():
        for peer in peers:
            pl.semaphore_signal(barrier, inc=1, device_id=peer, device_id_type=MESH)

    smalls = [pltpu.make_async_copy(src, dst, small_sem.at[n]) for n, (src, dst) in enumerate((
        (e_hbm, e_ref), (st_hbm, st_ref), (bin_hbm, bin_ref), (tap_hbm, tap_ref), (skip_hbm, skip_ref), (bout_hbm, bout_ref),
        (h_hbm.at[:, :, :, pl.ds(0, LANES)], lag_ref)))]
    first = pl.multiple_of(lax.rem(5 - sp, 3) * shard_len, LANES)

    def chunk_copies(layer, k):
        rows = pl.ds(k * rows_per if isinstance(k, int) else pl.multiple_of(k * rows_per, rows_per), rows_per)
        return [
            pltpu.make_async_copy(v_hbm.at[layer, :, rows, :], v_ref.at[layer, :, rows, :], chunk_sem.at[layer, k, 0]),
            pltpu.make_async_copy(z_hbm.at[layer, :, rows, :], z_ref.at[layer, :, rows, :], chunk_sem.at[layer, k, 1]),
            pltpu.make_async_copy(h_hbm.at[layer, :, rows, pl.ds(first, shard_len + LANES)], h_ref.at[layer, :, rows, :],
                                  chunk_sem.at[layer, k, 2]),
        ]

    def weight_copy(layer, n):
        src, dst = ((win_hbm, win), (wout_hbm, wout), (wup_hbm, wup), (wdown_hbm, wdown))[n]
        return pltpu.make_async_copy(src.at[layer], dst.at[layer], w_sem.at[layer, n])

    def start_weights(layer):
        @pl.when(carries)
        def _():
            for n in range(4):
                weight_copy(layer, n).start()

    for n in range(LAYERS * CHUNKS):
        layer, k = divmod(n, CHUNKS)
        for copy in chunk_copies(layer, k):
            copy.start()
        if n == CHUNKS:
            for copy in smalls:
                copy.start()
            start_weights(0)
    start_weights(1)

    lane8 = lax.broadcasted_iota(jnp.int32, (8, LANES), 1)
    lane16 = lax.broadcasted_iota(jnp.int32, (16, LANES), 1)
    spans = range(-1, tiles)

    def turn(cache, layer, row, dst):
        zero = jnp.zeros((16, LANES), jnp.bfloat16)

        def values(b, m):
            return cache[layer, b, pl.ds(row, 16), LANES * m:LANES * (m + 1)] if 0 <= m < tiles else zero

        parts = [jnp.concatenate([values(b, m), values(b, m + 1)], axis=1) for m in spans for b in range(SEQ)]
        dst[...] = jnp.dot(jnp.concatenate(parts, axis=0), flip[...], preferred_element_type=jnp.float32)

    def gather(layer, which, row, src):
        for u in range(2):
            accs = [[None] * SEQ for _ in range(STEPS)]
            after = None
            for m in spans:
                even = h_ref[layer, which, pl.ds(row + 8 * u, 8), LANES * (tiles - 1 - m):LANES * (tiles - m)]
                rolled = pltpu.roll(even, LANES - 1, 1)
                odd = rolled if after is None else jnp.where(lane8 < LANES - 1, rolled, after)
                after = rolled
                for b in range(SEQ):
                    base = 16 * (SEQ * (m + 1) + b) + 8 * u
                    for two in range(2):
                        value = src[base:base + 8, LANES * two:LANES * (two + 1)]
                        for one, taps in enumerate((even, odd)):
                            part = taps * value
                            j = 2 * two + one
                            accs[j][b] = part if accs[j][b] is None else accs[j][b] + part
            for j in range(STEPS):
                for b in range(SEQ):
                    n = SEQ * j + b
                    acc[which, pl.ds(row + 8 * u, 8), LANES * n:LANES * (n + 1)] = accs[j][b]

    def close(row):
        out = jnp.zeros((16, LANES), jnp.float32)
        for which in range(2):
            for j in range(STEPS):
                for b in range(SEQ):
                    n = SEQ * j + b
                    part = jnp.sum(acc[which, pl.ds(row, 16), LANES * n:LANES * (n + 1)], axis=1, keepdims=True)
                    out = jnp.where(lane16 == (2 * b + which) * STEPS + j, part, out)
        total[pl.ds(row, 16), :] = out

    def row_of(k):
        return k * 16 if isinstance(k, int) else pl.multiple_of(k * 16, 16)

    def conv(layer, p0, p1):
        def pair(p, _):
            k = 2 * p
            step = layer * CHUNKS + k + 2
            later, after = lax.rem(lax.div(step, CHUNKS), LAYERS), lax.rem(step, CHUNKS)
            for copy in chunk_copies(layer, k + 1):
                copy.wait()

            @pl.when(step < LAYERS * CHUNKS)
            def _():
                for copy in chunk_copies(later, after):
                    copy.wait()

            @pl.when(has_rows)
            def _():
                r0, r1, r2 = row_of(k), row_of(k + 1), row_of(after)
                turn(v_ref, layer, r1, v_odd)
                gather(layer, 0, r0, v_even)
                turn(z_ref, layer, r1, z_odd)
                gather(layer, 1, r0, z_even)
                turn(v_ref, later, r2, v_even)
                gather(layer, 0, r1, v_odd)
                turn(z_ref, later, r2, z_even)
                gather(layer, 1, r1, z_odd)

            return 0

        lax.fori_loop(p0, p1, pair, 0)

    lane_c = lax.broadcasted_iota(jnp.int32, (chan, LANES), 1)

    def hist_copy(layer, seq):
        return pltpu.make_async_remote_copy(hx.at[layer, sp, seq], hx.at[layer, sp, seq], hsend.at[layer, seq], hrecv.at[layer, sp],
                                            device_id={"sp": 2 * seq + 1}, device_id_type=MESH)

    def send_hist(layer):
        for row in range(0, chan, 16):
            close(row)
        turned = jnp.transpose(total[...])
        for b in range(SEQ):
            hx[layer, sp, b] = turned[2 * STEPS * b:2 * STEPS * (b + 1)]
        hist_copy(layer, 1).start()

        @pl.when(sp != 1)
        def _():
            hist_copy(layer, 0).start()

    def sum_hist(layer):
        for src in range(3):
            @pl.when(sp != src)
            def _():
                pltpu.make_async_remote_copy(hx.at[layer, src, own], hx.at[layer, src, own], hsend.at[layer, 0], hrecv.at[layer, src],
                                             device_id=block_peers[0], device_id_type=MESH).wait_recv()
        return (hx[layer, 0, own] + hx[layer, 1, own]) + hx[layer, 2, own]

    def sum_copies(n):
        return [pltpu.make_async_remote_copy(ar.at[n, tp], ar.at[n, tp], asend.at[n, d], arecv.at[n, tp],
                                             device_id=peers[d], device_id_type=MESH) for d in range(3)]

    def send_sum(n, part):
        ar[n, tp] = part
        for copy in sum_copies(n):
            copy.start()

    def take_sum(n):
        for d in (1, 2, 3):
            src = lax.rem(tp + d, 4)
            pltpu.make_async_remote_copy(ar.at[n, src], ar.at[n, src], asend.at[n, 0], arecv.at[n, src],
                                         device_id=peers[0], device_id_type=MESH).wait_recv()
        return ((ar[n, 0] + ar[n, 1]) + ar[n, 2]) + ar[n, 3]

    def row_copy(layer, seq, d):
        return pltpu.make_async_remote_copy(xb.at[layer, seq], xb.at[layer, seq], xsend.at[layer, d], xrecv.at[layer, seq],
                                            device_id=block_peers[d], device_id_type=MESH)

    def row_copies(layer, seq):
        return [row_copy(layer, seq, d) for d in range(3)]

    def last_copy(seq, d):
        return pltpu.make_async_remote_copy(fin.at[seq], fin.at[seq], fsend.at[d], frecv.at[seq],
                                            device_id=block_peers[d], device_id_type=MESH)

    def last_copies(seq):
        return [last_copy(seq, d) for d in range(3)]

    def project(layer, hidden):
        normed = layer_norm(hidden).astype(jnp.bfloat16)
        mixed = []
        for g in range(3):
            p = lax.dot_general(normed, win[layer, g], (((1,), (1,)), ((), ())), preferred_element_type=jnp.float32)
            p = (p + bin_ref[g, layer][None]).astype(jnp.bfloat16).astype(jnp.float32)
            prow[layer, g, 0:2, :] = st_ref[layer, own, g].astype(jnp.float32)
            prow[layer, g, 2:2 + STEPS, :] = p
            mixed.append(tap_ref[0, g, layer][None] * p + tap_ref[1, g, layer][None] * prow[layer, g, 1:1 + STEPS, :]
                         + tap_ref[2, g, layer][None] * prow[layer, g, 0:STEPS, :])
        return mixed

    def recent(layer, which, rows_f):
        rrow[layer, which, STEPS - 1:2 * STEPS - 1, :] = rows_f
        total = (lag[layer, which, 0:1] + skip_ref[layer, which][None]) * rows_f
        for back in range(1, STEPS):
            total = total + lag[layer, which, back:back + 1] * rrow[layer, which, STEPS - 1 - back:2 * STEPS - 1 - back, :]
        return total

    def mixer(layer, mixed, hist):
        value = mixed[2].astype(jnp.bfloat16).astype(jnp.float32)
        long_one = hist[:STEPS] + recent(layer, 0, value)
        z_rows = (mixed[0] * long_one).astype(jnp.bfloat16).astype(jnp.float32)
        long_two = hist[STEPS:] + recent(layer, 1, z_rows)
        y_rows = (mixed[1] * long_two).astype(jnp.bfloat16)
        send_sum(2 * layer, jnp.dot(y_rows, wout[layer], preferred_element_type=jnp.float32))
        for g in range(3):
            xb[layer, own, 2 * g:2 * g + 2, :] = prow[layer, g, STEPS:STEPS + 2, :]
        xb[layer, own, 6:8, :] = jnp.zeros((2, chan), jnp.float32)
        xb[layer, own, 8:8 + STEPS, :] = value
        xb[layer, own, 8 + STEPS:8 + 2 * STEPS, :] = z_rows
        for copy in row_copies(layer, own):
            copy.start()

    def mlp(layer, hidden):
        up = jnp.dot(layer_norm(hidden).astype(jnp.bfloat16), wup[layer], preferred_element_type=jnp.float32)
        return jnp.dot(jax.nn.gelu(up).astype(jnp.bfloat16), wdown[layer], preferred_element_type=jnp.float32)

    def put_rows(layer):
        for b in range(SEQ):
            @pl.when(sp != 2 * b + 1)
            def _():
                row_copy(layer, b, 0).wait_recv()

        for b in range(SEQ):
            newrow[2 * STEPS * b:2 * STEPS * (b + 1), 0:chan] = xb[layer, b, 8:16, :]
            for g in range(3):
                st_out[layer, b, g] = xb[layer, b, 2 * g:2 * g + 2, :].astype(jnp.bfloat16)
        turned = jnp.transpose(newrow[...])[:chan]

        @pl.when(sp == 3)
        def _():
            for b in range(SEQ):
                for n, cache in enumerate((v_ref, z_ref)):
                    at = STEPS * (2 * b + n)
                    moved = turned if at == 0 else pltpu.roll(turned, LANES - at, 1)
                    cache[layer, b, :, 0:LANES] = jnp.where(lane_c < STEPS, moved, 0.0).astype(jnp.bfloat16)

    newrow[...] = jnp.zeros_like(newrow)
    rrow[...] = jnp.zeros_like(rrow)
    kk = lax.broadcasted_iota(jnp.int32, flip.shape, 0)
    nn = lax.broadcasted_iota(jnp.int32, flip.shape, 1)
    flip[...] = jnp.where(kk == jnp.where(nn < LANES, LANES - nn, 2 * LANES + 2 - nn), 1.0, 0.0).astype(jnp.bfloat16)
    head = chunk_copies(0, 0)
    head[0].wait()
    head[1].wait()

    @pl.when(has_rows)
    def _():
        turn(v_ref, 0, 0, v_even)
        turn(z_ref, 0, 0, z_even)

    head[2].wait()

    def stage(n, _):
        at_least = [None] + [lax.div(n + 3 - i, 3) if i == 1 else lax.div(n, i) for i in (1, 2, 3)]
        conv(at_least[1], FIRST * at_least[2] + SECOND * at_least[3],
             CHUNKS // 2 - (CHUNKS // 2 - FIRST) * (at_least[1] - at_least[2])
             - (CHUNKS // 2 - FIRST - SECOND) * (at_least[2] - at_least[3]))

        @pl.when((n == 0) & carries)
        def _():
            pl.semaphore_wait(barrier, 6)

        @pl.when((n == 0) & jnp.logical_not(carries))
        def _():
            pl.semaphore_wait(barrier, 3)

        @pl.when(((n == 0) | (n == 3)) & has_rows)
        def _():
            send_hist(lax.div(n, 3))

        @pl.when(n == 0)
        def _():
            for copy in smalls:
                copy.wait()

        @pl.when((n == 0) & carries)
        def _():
            hidden = jnp.where(own == 0, jnp.concatenate([e_ref[j].astype(jnp.float32)[0:1] for j in range(STEPS)], axis=0),
                               jnp.concatenate([e_ref[j].astype(jnp.float32)[1:2] for j in range(STEPS)], axis=0))
            held[...] = hidden
            weight_copy(0, 0).wait()
            for g, rows_f in enumerate(project(0, hidden)):
                mixed_ref[g] = rows_f
            for layer in range(LAYERS):
                for which in range(2):
                    lag[layer, which] = jnp.transpose(lag_ref[layer, which])[:8]
            for n_w in (1, 2, 3):
                weight_copy(0, n_w).wait()

        @pl.when((n == 1) & carries)
        def _():
            mixer(0, [mixed_ref[g] for g in range(3)], sum_hist(0))

        @pl.when((n == 2) & carries)
        def _():
            hidden = held[...] + take_sum(0) + bout_ref[0:1]
            send_sum(1, mlp(0, hidden))
            held[...] = hidden

        return 0

    lax.fori_loop(0, 4, stage, 0)

    @pl.when(carries)
    def _():
        weight_copy(1, 0).wait()
        hidden = held[...] + take_sum(1)
        mixed = project(1, hidden)
        weight_copy(1, 1).wait()
        mixer(1, mixed, sum_hist(1))
        put_rows(0)
        weight_copy(1, 2).wait()
        weight_copy(1, 3).wait()
        hidden = hidden + take_sum(2) + bout_ref[1:2]
        send_sum(3, mlp(1, hidden))
        put_rows(1)
        fin[own] = hidden + take_sum(3)
        for copy in last_copies(own):
            copy.start()
        for layer in range(LAYERS):
            for copy in row_copies(layer, own):
                copy.wait_send()
        for n in range(4):
            for copy in sum_copies(n):
                copy.wait_send()
        for copy in last_copies(own):
            copy.wait_send()

    @pl.when(jnp.logical_not(carries))
    def _():
        put_rows(0)
        put_rows(1)

    for layer in range(LAYERS):
        @pl.when(has_rows)
        def _():
            hist_copy(layer, 1).wait_send()

            @pl.when(sp != 1)
            def _():
                hist_copy(layer, 0).wait_send()

    for b in range(SEQ):
        @pl.when(sp != 2 * b + 1)
        def _():
            last_copy(b, 0).wait_recv()

        for j in range(STEPS):
            hid_out[j, b:b + 1, :] = fin[b, j:j + 1, :]


def emit(hid, v, z, st, hid_o, v_o, z_o, st_o, sem):
    copies = []
    copies = [(hid, hid_o), (st, st_o)]
    for layer in range(LAYERS):
        copies += [(v.at[layer], v_o.at[layer]), (z.at[layer], z_o.at[layer])]
    copies = [pltpu.make_async_copy(src, dst, sem.at[n]) for n, (src, dst) in enumerate(copies)]
    for copy in copies:
        copy.start()
    for copy in copies:
        copy.wait()


def solution(mesh):
    def device_fn(step_emb, v_cache, z_cache, short_state, w_in, b_in, short_taps, long_filt, skip_gain, w_out, b_out, w_up, w_down):
        chan = v_cache.shape[3]
        shard_len = v_cache.shape[2]
        model = step_emb.shape[2]
        args = (
            step_emb,
            jnp.swapaxes(v_cache, 2, 3),
            jnp.swapaxes(z_cache, 2, 3),
            jnp.transpose(short_state, (0, 1, 3, 2, 4)),
            jnp.transpose(w_in, (0, 2, 3, 1)),
            jnp.transpose(b_in, (1, 0, 2)),
            jnp.transpose(short_taps, (1, 2, 0, 3)),
            jnp.swapaxes(long_filt, 2, 3),
            skip_gain,
            w_out,
            b_out,
            w_up,
            w_down,
        )
        args = tuple(pltpu.with_memory_space_constraint(arg, pltpu.HBM) for arg in args)
        f32, bf16 = jnp.float32, jnp.bfloat16
        dma = pltpu.SemaphoreType.DMA
        hid, v_out, z_out, st_out = pl.pallas_call(
            kernel,
            out_shape=(
                jax.ShapeDtypeStruct(step_emb.shape, f32),
                pltpu.VMEM(args[1].shape, bf16),
                pltpu.VMEM(args[2].shape, bf16),
                jax.ShapeDtypeStruct(args[3].shape, bf16),
            ),
            in_specs=[pl.BlockSpec(memory_space=pltpu.HBM)] * 13,
            out_specs=[pl.BlockSpec(memory_space=pltpu.VMEM)] * 4,
            scratch_shapes=[
                pltpu.VMEM(step_emb.shape, bf16),
                pltpu.VMEM(args[3].shape, bf16),
                pltpu.VMEM(args[4].shape, bf16),
                pltpu.VMEM(args[5].shape, f32),
                pltpu.VMEM(args[6].shape, f32),
                pltpu.VMEM((LAYERS, 2, chan, shard_len + LANES), f32),
                pltpu.VMEM((LAYERS, 2, chan, LANES), f32),
                pltpu.VMEM(skip_gain.shape, f32),
                pltpu.VMEM(w_out.shape, bf16),
                pltpu.VMEM(b_out.shape, f32),
                pltpu.VMEM(w_up.shape, bf16),
                pltpu.VMEM(w_down.shape, bf16),
                pltpu.VMEM((2 * LANES, 2 * LANES), bf16),
                *[pltpu.VMEM((16 * SEQ * (shard_len // LANES + 1), 2 * LANES), f32)] * 4,
                pltpu.VMEM((2, chan, ROWS * LANES), f32),
                pltpu.VMEM((chan, LANES), f32),
                pltpu.VMEM((LAYERS, 2, 8, chan), f32),
                pltpu.VMEM((LAYERS, 3, 8, chan), f32),
                pltpu.VMEM((LAYERS, 2, 8, chan), f32),
                pltpu.VMEM((LANES, 2 * LANES), f32),
                pltpu.VMEM((LAYERS, 4, SEQ, 2 * STEPS, chan), f32),
                pltpu.VMEM((4, 4, STEPS, model), f32),
                pltpu.VMEM((LAYERS, SEQ, 16, chan), f32),
                pltpu.VMEM((SEQ, STEPS, model), f32),
                pltpu.VMEM((STEPS, model), f32),
                pltpu.VMEM((3, STEPS, chan), f32),
                dma((7,)),
                dma((LAYERS, CHUNKS, 3)),
                dma((LAYERS, 4)),
                dma((LAYERS, SEQ)),
                dma((LAYERS, 4)),
                dma((4, 3)),
                dma((4, 4)),
                dma((LAYERS, 3)),
                dma((LAYERS, SEQ)),
                dma((3,)),
                dma((SEQ,)),
            ],
            compiler_params=pltpu.CompilerParams(collective_id=0, has_side_effects=True, vmem_limit_bytes=40 * 1024 * 1024),
            name="decode",
        )(*args)
        hid, v_out, z_out, st_out = pl.pallas_call(
            emit,
            out_shape=(
                jax.ShapeDtypeStruct(hid.shape, f32),
                jax.ShapeDtypeStruct(v_out.shape, bf16),
                jax.ShapeDtypeStruct(z_out.shape, bf16),
                jax.ShapeDtypeStruct(st_out.shape, bf16),
            ),
            in_specs=[pl.BlockSpec(memory_space=pltpu.VMEM)] * 4,
            out_specs=[pl.BlockSpec(memory_space=pltpu.HBM)] * 4,
            scratch_shapes=[dma((2 * LAYERS + 2,))],
            compiler_params=pltpu.CompilerParams(vmem_limit_bytes=1024 * 1024),
            name="emit",
        )(hid, v_out, z_out, st_out)
        return (hid, jnp.swapaxes(v_out, 2, 3), jnp.swapaxes(z_out, 2, 3), jnp.transpose(st_out, (0, 1, 3, 2, 4)))

    specs_in = (
        P(None, "dp", None),
        P(None, "dp", "sp", "tp"),
        P(None, "dp", "sp", "tp"),
        P(None, "dp", None, None, "tp"),
        P(None, None, None, "tp"),
        P(None, None, "tp"),
        P(None, None, None, "tp"),
        P(None, None, None, "tp"),
        P(None, None, "tp"),
        P(None, "tp", None),
        P(None, None),
        P(None, None, "tp"),
        P(None, "tp", None),
    )
    specs_out = (
        P(None, "dp", None),
        P(None, "dp", "sp", "tp"),
        P(None, "dp", "sp", "tp"),
        P(None, "dp", None, None, "tp"),
    )
    return jax.shard_map(device_fn, mesh=mesh, in_specs=specs_in, out_specs=specs_out, check_vma=False)
```
